32 devices in a mesh: field: 2 (over x), ep: 16 (over z, y, core).
Axes of the slice: x: 2, y: 2, z: 4, core: 2. Of those that a mesh axis runs over, the one named last changes fastest.
Arguments:
- images: float32 [64, 16, 256], P(('field', 'ep')), parts along dimension 0, may hold values from -6 to 6
- reference_image: float32 [32, 256], P('field'), parts along dimension 0, may hold values from -6 to 6
- kernels: float32 [16, 23, 23], replicated, may hold values from -0.25 to 0.25
- kernel_index: int32 [64], P(('field', 'ep')), parts along dimension 0, may hold values from 0 to 15
- tile_mask: int32 [64, 16, 2], P(('field', 'ep')), parts along dimension 0, may hold values 0 or 1
- systematics: float32 [64, 40], P('field'), parts along dimension 0, may hold values from -6 to 6
- onsets: int32 [16], P('field'), parts along dimension 0, may hold values from 0 to 27
Outputs:
- coefficients: float32 [48, 32, 256], P(None, ('field', 'ep')), parts along dimension 1
- epoch_scatter: float32 [64], P('field'), parts along dimension 0
The draws below stay inside these ranges and needn't reach their ends.
There are 2 independent parts, one for each index of `field`. The reference program is written for one: setup_inputs(seed, part) draws one part's arguments, and reference() takes and returns one part's arrays. A program takes and returns all parts, laid end to end along the dimension named above; an argument that names none is the same for every part. Nothing has to cross between parts.
All inputs are finite; a program needn't handle non-finite values. No bound on the sum of `tile_mask` on one device may be relied on, other than what follows from the above.
Results may differ from the reference program's by a relative error of at most 0.00011.
Values sent between devices are 32-bit elements; how exact they have to be, the bound alone decides.
A program may use at most 64 MiB of HBM per device.

```python
import jax
import jax.numpy as jnp
from jax import lax

W = 256
KS = 23
NK = 16
NSYS = 40
NTR = 8
R = 16
E = 32


def touch_ends(drawn, stream_key, smallest, high):
    dims = drawn.shape
    spot = [jax.random.randint(jax.random.fold_in(stream_key, axis), (), 0, dims[axis]) for axis in range(len(dims))]
    drawn = drawn.at[tuple(spot)].set(smallest)
    longest = dims.index(max(dims))
    spot[longest] = (spot[longest] + 1) % dims[longest]
    return drawn.at[tuple(spot)].set(high)


def block_levels(rng, dims, cuts, least, largest):
    level, own = 1.0, jax.random.fold_in(rng, 6)
    for position, shards_of in cuts:
        steps = jnp.exp(jax.random.uniform(jax.random.fold_in(own, position), (shards_of,), jnp.float32, least / len(cuts), largest / len(cuts)))
        level = level * jnp.repeat(steps, dims[position] // shards_of).reshape([-1 if axis == position else 1 for axis in range(len(dims))])
    return level


def noise(stream_key, dims, scale, reach, shards=(), kind=jnp.bfloat16):
    factor_of = block_levels(stream_key, dims, shards, -0.22, 0.18) if shards else 1.0
    values = jax.random.normal(stream_key, dims, jnp.float32) * scale * factor_of
    return jnp.minimum(jnp.maximum(values, -reach), reach).astype(kind)


def setup_inputs(seed: int = 0, part: int = 0) -> dict:
    splits = jax.random.split(jax.random.key(seed), 8)
    own_keys = jax.random.split(jax.random.fold_in(splits[7], part), 8)
    images = noise(own_keys[0], (E, R, W), 1.0, 6.0, ((0, 16),), jnp.float32)
    reference_image = noise(own_keys[1], (R, W), 1.0, 6.0, (), jnp.float32)
    kernels = noise(splits[2], (NK, KS, KS), (KS * KS) ** -0.5, 0.25, (), jnp.float32)
    kernel_index = touch_ends(jax.random.randint(own_keys[3], (E,), 0, NK), jax.random.fold_in(own_keys[3], 1), 0, NK - 1).astype(jnp.int32)
    tile_mask = touch_ends((jax.random.randint(own_keys[4], (E, R, W // 128), 0, 8) < 7).astype(jnp.int32), jax.random.fold_in(own_keys[4], 1), 0, 1)
    systematics = noise(own_keys[5], (E, NSYS), 1.0, 6.0, (), jnp.float32)
    onsets = touch_ends(jax.random.randint(own_keys[6], (NTR,), 0, E - 4), jax.random.fold_in(own_keys[6], 1), 0, (E - 4) - 1).astype(jnp.int32)
    return dict(images=images, reference_image=reference_image, kernels=kernels, kernel_index=kernel_index, tile_mask=tile_mask, systematics=systematics, onsets=onsets)


cov_ridge = 0.5
fit_ridge = 1.0

def correlate(stack, chosen):
    count = stack.shape[0]
    filters = jnp.transpose(chosen, (1, 2, 0))[:, :, None, :]
    result = lax.conv_general_dilated(stack[None], filters, (1, 1), 'SAME', dimension_numbers=('NCHW', 'HWIO', 'NCHW'), feature_group_count=count, precision=lax.Precision.HIGHEST)
    return result[0]

def subtract(stack, reference_image, chosen, masks):
    result = reference_image[None] - correlate(stack, chosen)
    shape = result.shape
    tiles = result.reshape(shape[0], shape[1], shape[2] // 128, 128) * masks[..., None].astype(jnp.float32)
    return tiles.reshape(shape)

def build_design(systematics, onsets):
    count = systematics.shape[0]
    templates = onsets.shape[0]
    epoch_axis = jnp.arange(count, dtype=jnp.float32)[:, None]
    delays = epoch_axis - onsets[None, :].astype(jnp.float32)
    timescale = (jnp.arange(templates, dtype=jnp.float32) + 1.0) * count / (2.0 * templates)
    transient = jnp.where(delays >= 0.0, jnp.exp(-jnp.maximum(delays, 0.0) / timescale[None, :]), 0.0)
    return jnp.concatenate([systematics, transient.astype(systematics.dtype)], axis=1)

def fit_matrix(scatter, npixels, design):
    count = design.shape[0]
    columns = design.shape[1]
    covariance = scatter / npixels + cov_ridge * jnp.eye(count, dtype=scatter.dtype)
    lower = jnp.linalg.cholesky(covariance)
    weighted = jax.scipy.linalg.cho_solve((lower, True), design)
    normal = jnp.dot(design.T, weighted, precision=lax.Precision.HIGHEST) + fit_ridge * jnp.eye(columns, dtype=scatter.dtype)
    lower_fit = jnp.linalg.cholesky(normal)
    return jax.scipy.linalg.cho_solve((lower_fit, True), weighted.T)

def reference(images, reference_image, kernels, kernel_index, tile_mask, systematics, onsets):
    count, rows, width = images.shape
    chosen = kernels[kernel_index]
    difference = subtract(images, reference_image, chosen, tile_mask)
    pixel_data = difference.reshape(count, rows * width)
    scatter = jnp.dot(pixel_data, pixel_data.T, precision=lax.Precision.HIGHEST)
    npixels = float(rows * width)
    design = build_design(systematics, onsets)
    fit = fit_matrix(scatter, npixels, design)
    coefficients = jnp.dot(fit, pixel_data, precision=lax.Precision.HIGHEST)
    residual = pixel_data - jnp.dot(design, coefficients, precision=lax.Precision.HIGHEST)
    epoch_scatter = jnp.sum(residual * residual, axis=1) / npixels
    return (coefficients.reshape(design.shape[1], rows, width), epoch_scatter)
```

```python
import functools

import jax
import jax.numpy as jnp
from jax import lax
from jax.experimental import pallas as pl
from jax.experimental.pallas import tpu as pltpu
from jax.sharding import PartitionSpec as P

cov_ridge = 0.5
fit_ridge = 1.0
LANES = 128
VMEM_GRANT = 24 * 2**20
HIGHEST = lax.Precision.HIGHEST


def dot(a, b, contract):
    return lax.dot_general(
        a, b, ((contract[0], contract[1]), ((), ())), precision=HIGHEST, preferred_element_type=jnp.float32
    )


def iota(shape, axis):
    return lax.broadcasted_iota(jnp.int32, shape, axis)


def exchange_kernel(
    n,
    hubs,
    images_hbm,
    reference_hbm,
    kernels_hbm,
    index_hbm,
    mask_hbm,
    systematics_hbm,
    onsets_hbm,
    pixels,
    total_ref,
    work,
    images_ref,
    reference_ref,
    kernels_ref,
    index_ref,
    mask_ref,
    systematics_ref,
    onsets_ref,
    table,
    table_t,
    taps,
    shifted,
    send,
    recv,
    part,
    parts,
    load_sem,
    row_sem,
    hub_sem,
    part_sem,
    hub_send_sem,
    row_send_sem,
    part_send_sem,
):
    local, rows, width = images_ref.shape
    side = kernels_ref.shape[0]
    half = (side - 1) // 2
    tiles = width // LANES
    block = rows // n
    epochs = local * n
    nsys = systematics_ref.shape[1]
    ntr = onsets_ref.shape[0]
    columns = nsys + ntr
    pack = max(LANES // epochs, 1)
    me = lax.axis_index("ep")
    count = len(hubs)
    pieces = recv.shape[0]
    strips = block * tiles

    loads = [
        pltpu.make_async_copy(source, target, load_sem.at[i])
        for i, (source, target) in enumerate(
            (
                (index_hbm, index_ref),
                (kernels_hbm, kernels_ref),
                (images_hbm, images_ref),
                (mask_hbm, mask_ref),
                (reference_hbm, reference_ref),
                (systematics_hbm, systematics_ref),
                (onsets_hbm, onsets_ref),
            )
        )
    ]
    for load in loads:
        load.start()

    barrier = pltpu.get_barrier_semaphore()
    for d in range(1, n):
        pl.semaphore_signal(
            barrier,
            inc=1,
            device_id={"ep": lax.rem(me + d, n)},
            device_id_type=pl.DeviceIdType.MESH,
        )
    for load in loads:
        load.wait()

    depth = side * rows
    padded_depth = taps.shape[1]
    lane = iota((rows, LANES), 1)
    column = iota((rows, width), 1)
    for e in range(local):
        table[...] = jnp.zeros_like(table)
        for a in range(side):
            table[a : a + 1, 0:side] = kernels_ref[a, pl.ds(index_ref[e], 1), :]
        table[side + 1 : side + 1 + tiles, 0:rows] = mask_ref[e].astype(jnp.float32)
        table_t[...] = table[...].T
        kept = jnp.where(iota((side, LANES), 1) < side, table_t[0:side, :], 0.0)
        kept = pltpu.roll(kept, LANES - half, axis=1)
        groups = [jnp.zeros((rows, LANES), jnp.float32) for _ in range(padded_depth // LANES)]
        for b in range(side):
            start = b * rows
            at = start % LANES
            row = jnp.broadcast_to(kept[b : b + 1, :], (rows, LANES))
            turned = pltpu.roll(row, at, axis=1, stride=1, stride_axis=0)
            inside = (lane >= at) & (lane < at + rows)
            groups[start // LANES] = jnp.where(inside, turned, groups[start // LANES])
        for g, value in enumerate(groups):
            taps[:, g * LANES : (g + 1) * LANES] = value
        image = images_ref[e]
        for b in range(side):
            move = b - half
            moved = pltpu.roll(image, (-move) % width, axis=1) if move else image
            inside = (column + move >= 0) & (column + move < width)
            shifted[b * rows : (b + 1) * rows, :] = jnp.where(inside, moved, 0.0)
        if padded_depth > depth:
            shifted[depth:, :] = jnp.zeros((padded_depth - depth, width), jnp.float32)
        difference = reference_ref[...] - dot(taps[...], shifted[...], ((1,), (0,)))
        for t in range(tiles):
            good = table_t[0:rows, side + 1 + t : side + 2 + t]
            piece = difference[:, t * LANES : (t + 1) * LANES] * good
            for r in range(0, rows, 8):
                first = (r * tiles + t) * local + e
                send[pl.ds(first, 8, stride=tiles * local), :] = piece[r : r + 8, :]

    sources = send.reshape(rows * tiles, local, LANES)
    pl.semaphore_wait(barrier, n - 1)

    def copy(source, target, semaphores, device):
        send_semaphore, semaphore = semaphores
        return pltpu.make_async_remote_copy(
            src_ref=source,
            dst_ref=target,
            send_sem=send_semaphore,
            recv_sem=semaphore,
            device_id={"ep": device},
            device_id_type=pl.DeviceIdType.MESH,
        )

    for k, hub in enumerate(hubs):
        mine = sources.at[k * pieces : (k + 1) * pieces]

        @pl.when(me != hub)
        def _():
            copy(mine, recv.at[:, me], (hub_send_sem, hub_sem), hub).start()

        @pl.when(me == hub)
        def _():
            recv[:, me] = mine[...]

    for d in range(1, n):
        device = lax.rem(me + d, n)
        rows_of = sources.at[pl.ds(device * strips, strips)]
        copy(rows_of, pixels.at[:, me], (row_send_sem, row_sem), device).start()
    pixels[:, me] = sources[pl.ds(me * strips, strips)]

    work[...] = jnp.zeros_like(work)
    epoch = iota((epochs, LANES), 0).astype(jnp.float32)
    template = iota((epochs, LANES), 1)
    onset = jnp.zeros((epochs, LANES), jnp.float32)
    for k in range(ntr):
        onset = jnp.where(template == k, onsets_ref[k].astype(jnp.float32), onset)
    delays = epoch - onset
    timescale = (template.astype(jnp.float32) + 1.0) * epochs / (2.0 * ntr)
    transient = jnp.where(delays >= 0.0, jnp.exp(-jnp.maximum(delays, 0.0) / timescale), 0.0)
    work[:, epochs : epochs + nsys] = systematics_ref[...]
    work[:, epochs + nsys : epochs + columns] = transient[:, 0:ntr]
    design = work[...]
    outer = dot(design, design, ((1,), (1,)))
    diagonal = iota((epochs, epochs), 0) == iota((epochs, epochs), 1)
    ridge = jnp.where(diagonal, cov_ridge, 0.0)
    work[:, 0:epochs] = fit_ridge * outer + ridge
    work[:, epochs + columns : 2 * epochs + columns] = ridge

    def drain(ref, semaphore):
        pltpu.make_async_copy(ref, ref, semaphore).wait()

    def hub_work(k):
        others = recv.at[:, 0 : n - 1]
        drain(others, hub_sem)
        gathered = recv.reshape(pieces, epochs, LANES)
        step = min(pieces, 32)

        def gram(start):
            data = jnp.concatenate([gathered[start + i] for i in range(step)], axis=1)
            return dot(data, data, ((1,), (1,)))

        if step == pieces:
            partial_scatter = gram(0)
        else:
            partial_scatter = lax.fori_loop(
                0,
                pieces // step,
                lambda i, value: value + gram(i * step),
                jnp.zeros((epochs, epochs), jnp.float32),
            )
        share = epochs // pack
        if pack > 1:
            table[0:epochs, :] = jnp.zeros((epochs, LANES), jnp.float32)
            table[0:epochs, 0:epochs] = partial_scatter
            wide = table[0:epochs, :]
            packed = wide[0:share, :]
            for j in range(1, pack):
                packed = packed + pltpu.roll(
                    wide[j * share : (j + 1) * share, :], j * epochs, axis=1
                )
            part[...] = packed
        else:
            part[...] = partial_scatter
        for d in range(1, n):
            device = lax.rem(me + n - d, n)
            copy(part, parts.at[k], (part_send_sem, part_sem), device).start()
        parts[k] = part[...]

    for k, hub in enumerate(hubs):

        @pl.when(me == hub)
        def _():
            hub_work(k)
            if count > 1:
                drain(parts.at[0 : count - 1], part_sem)

    is_hub = functools.reduce(jnp.logical_or, [me == hub for hub in hubs])

    @pl.when(jnp.logical_not(is_hub))
    def _():
        drain(parts.at[0:count], part_sem)

    total = parts[0]
    for j in range(1, count):
        total = total + parts[j]
    total_ref[...] = total
    drain(pixels.at[:, 0 : n - 1], row_sem)

    drain(pixels.at[:, 0 : n - 1], row_send_sem)

    @pl.when(jnp.logical_not(is_hub))
    def _():
        drain(sources.at[0 : count * pieces], hub_send_sem)

    @pl.when(is_hub)
    def _():
        if count > 1:
            drain(sources.at[0 : (count - 1) * pieces], hub_send_sem)
        drain(parts.at[0 : n - 1], part_send_sem)


def fit_kernel(npixels, pixels_ref, total_ref, base_ref, coefficients_ref, epoch_ref, work):
    columns, block, width = coefficients_ref.shape
    strips, n, local, _ = pixels_ref.shape
    epochs = n * local
    rows_of = pixels_ref.reshape(strips, epochs, LANES)
    data = jnp.concatenate([rows_of[i] for i in range(strips)], axis=1)
    pack = epochs // total_ref.shape[0]
    total = total_ref[...]
    if pack > 1:
        pieces = [total] + [
            pltpu.roll(total, LANES - j * epochs, axis=1) for j in range(1, pack)
        ]
        scatter = jnp.concatenate(pieces, axis=0)[:, 0:epochs]
    else:
        scatter = total

    covariance = scatter * (1.0 / npixels)
    work[...] = jnp.zeros_like(work)
    work[:, 0:epochs] = covariance
    work[:, epochs + columns : 2 * epochs + columns] = covariance
    system = work[...] + base_ref[...]
    lanes = system.shape[1]
    group = (8, lanes)
    strips = [system[i : i + 8, :] for i in range(0, epochs, 8)]
    index = iota(group, 0)

    def spread(value, row):
        return jnp.broadcast_to(value[row : row + 1, :], group)

    for home in range(epochs // 8):
        spans = [
            [jnp.broadcast_to(strip[:, k : k + 1], group) for strip in strips]
            for k in range(home * 8, home * 8 + 8)
        ]
        for row in range(0, 8, 2):
            lefts, rights = spans[row], spans[row + 1]
            a, b = spread(lefts[home], row), spread(rights[home], row)
            c, d = spread(lefts[home], row + 1), spread(rights[home], row + 1)
            inverse = 1.0 / (a * d - b * c)

            def step(values):
                first, second = spread(values[home], row), spread(values[home], row + 1)
                upper = (d * first - b * second) * inverse
                lower = (a * second - c * first) * inverse
                values = [
                    v - left * upper - right * lower
                    for v, left, right in zip(values, lefts, rights)
                ]
                values[home] = jnp.where(
                    index == row, upper, jnp.where(index == row + 1, lower, values[home])
                )
                return values

            spans = [step(span) if j > row + 1 else span for j, span in enumerate(spans)]
            strips = step(strips)
    system = jnp.concatenate(strips, axis=0)

    fitted = dot(system, data, ((0,), (0,)))[epochs : epochs + columns, :]
    for q in range(block):
        coefficients_ref[:, q, :] = fitted[:, q * width : (q + 1) * width]
    product = dot(scatter, system, ((1,), (0,))) * system
    work[0:1, :] = jnp.sum(product, axis=0, keepdims=True) * (1.0 / npixels)
    epoch_ref[...] = work[0, epochs + columns : 2 * epochs + columns]


HUBS = (1,)


def hub_devices(n):
    return HUBS


def ceil_to(value, unit):
    return -(-value // unit) * unit


def solution(mesh):
    n = mesh.shape["ep"]

    def shards(images, reference_image, kernels, kernel_index, tile_mask, systematics, onsets):
        local, rows, width = images.shape
        side = kernels.shape[1]
        tiles = width // LANES
        block = rows // n
        epochs = local * n
        columns = systematics.shape[1] + onsets.shape[0]
        pack = max(LANES // epochs, 1)
        share = epochs // pack
        part_lanes = max(LANES, epochs)
        vmem = pl.BlockSpec(memory_space=pltpu.VMEM)
        dma = pltpu.SemaphoreType.DMA
        f32 = jnp.float32
        flat_kernels = jnp.transpose(kernels, (1, 0, 2))
        flat_mask = jnp.transpose(tile_mask, (0, 2, 1))
        system_lanes = ceil_to(2 * epochs + columns, LANES)
        hubs = hub_devices(n)
        pieces = rows * tiles // len(hubs)
        strips = block * tiles
        pixels, total, base = pl.pallas_call(
            functools.partial(exchange_kernel, n, hubs),
            out_shape=(
                jax.ShapeDtypeStruct((strips, n, local, LANES), f32),
                jax.ShapeDtypeStruct((share, part_lanes), f32),
                jax.ShapeDtypeStruct((epochs, system_lanes), f32),
            ),
            in_specs=[pl.BlockSpec(memory_space=pltpu.HBM)] * 7,
            out_specs=(vmem, vmem, vmem),
            scratch_shapes=[
                pltpu.VMEM(images.shape, f32),
                pltpu.VMEM(reference_image.shape, f32),
                pltpu.VMEM(flat_kernels.shape, f32),
                pltpu.SMEM(kernel_index.shape, jnp.int32),
                pltpu.VMEM(flat_mask.shape, jnp.int32),
                pltpu.VMEM(systematics.shape, f32),
                pltpu.SMEM(onsets.shape, jnp.int32),
                pltpu.VMEM((LANES, LANES), f32),
                pltpu.VMEM((LANES, LANES), f32),
                pltpu.VMEM((rows, ceil_to(side * rows, LANES)), f32),
                pltpu.VMEM((ceil_to(side * rows, LANES), width), f32),
                pltpu.VMEM((rows * tiles * local, LANES), f32),
                pltpu.VMEM((pieces, n, local, LANES), f32),
                pltpu.VMEM((share, part_lanes), f32),
                pltpu.VMEM((n, share, part_lanes), f32),
                pltpu.SemaphoreType.DMA((7,)),
                dma,
                dma,
                dma,
                dma,
                dma,
                dma,
            ],
            compiler_params=pltpu.CompilerParams(
                collective_id=0, has_side_effects=True, vmem_limit_bytes=VMEM_GRANT
            ),
        )(
            *(
                pltpu.with_memory_space_constraint(value, pltpu.HBM)
                for value in (
                    images,
                    reference_image,
                    flat_kernels,
                    kernel_index,
                    flat_mask,
                    systematics,
                    onsets,
                )
            )
        )
        return pl.pallas_call(
            functools.partial(fit_kernel, float(rows * width)),
            out_shape=(
                jax.ShapeDtypeStruct((columns, block, width), f32),
                jax.ShapeDtypeStruct((epochs,), f32),
            ),
            in_specs=[vmem, vmem, vmem],
            out_specs=(vmem, vmem),
            scratch_shapes=[pltpu.VMEM((epochs, system_lanes), f32)],
            compiler_params=pltpu.CompilerParams(vmem_limit_bytes=VMEM_GRANT),
        )(pixels, total, base)

    in_specs = (
        P(("field", "ep"), None, None),
        P("field", None),
        P(),
        P(("field", "ep")),
        P(("field", "ep"), None, None),
        P("field", None),
        P("field"),
    )
    out_specs = (P(None, ("field", "ep"), None), P("field"))
    return jax.shard_map(shards, mesh=mesh, in_specs=in_specs, out_specs=out_specs, check_vma=False)
```

```python
import functools

import jax
import jax.numpy as jnp
from jax import lax
from jax.experimental import pallas as pl
from jax.experimental.pallas import tpu as pltpu
from jax.sharding import PartitionSpec as P

cov_ridge = 0.5
fit_ridge = 1.0
LANES = 128
VMEM_GRANT = 24 * 2**20
HIGHEST = lax.Precision.HIGHEST


def dot(a, b, contract):
    return lax.dot_general(
        a, b, ((contract[0], contract[1]), ((), ())), precision=HIGHEST, preferred_element_type=jnp.float32
    )


def iota(shape, axis):
    return lax.broadcasted_iota(jnp.int32, shape, axis)


def exchange_kernel(
    n,
    hub,
    images_hbm,
    reference_hbm,
    kernels_hbm,
    index_hbm,
    mask_hbm,
    systematics_hbm,
    onsets_hbm,
    pixels,
    total_ref,
    work,
    images_ref,
    reference_ref,
    kernels_ref,
    index_ref,
    mask_ref,
    systematics_ref,
    onsets_ref,
    table,
    table_t,
    taps,
    shifted,
    send,
    recv,
    spare,
    load_sem,
    ready_sem,
    row_sem,
    hub_sem,
    total_sem,
    hub_send_sem,
    row_send_sem,
    total_send_sem,
):
    local, rows, width = images_ref.shape
    side = kernels_ref.shape[0]
    half = (side - 1) // 2
    tiles = width // LANES
    block = rows // n
    epochs = local * n
    nsys = systematics_ref.shape[1]
    ntr = onsets_ref.shape[0]
    columns = nsys + ntr
    pack = max(LANES // epochs, 1)
    me = lax.axis_index("ep")
    mate = hub - 1
    pieces = recv.shape[0]
    strips = block * tiles

    loads = [
        pltpu.make_async_copy(source, target, load_sem.at[i])
        for i, (source, target) in enumerate(
            (
                (index_hbm, index_ref),
                (kernels_hbm, kernels_ref),
                (images_hbm, images_ref),
                (mask_hbm, mask_ref),
                (reference_hbm, reference_ref),
                (systematics_hbm, systematics_ref),
                (onsets_hbm, onsets_ref),
            )
        )
    ]
    for load in loads:
        load.start()

    def signal(semaphore, device):
        pl.semaphore_signal(
            semaphore, inc=1, device_id={"ep": device}, device_id_type=pl.DeviceIdType.MESH
        )

    barrier = pltpu.get_barrier_semaphore()

    @pl.when(me == hub)
    def _():
        for d in range(1, n):
            signal(barrier, lax.rem(me + d, n))

    @pl.when(me != hub)
    def _():
        signal(barrier, hub)

    for load in loads:
        load.wait()

    depth = side * rows
    padded_depth = taps.shape[1]
    lane = iota((rows, LANES), 1)
    column = iota((rows, width), 1)
    for e in range(local):
        table[...] = jnp.zeros_like(table)
        for a in range(side):
            table[a : a + 1, 0:side] = kernels_ref[a, pl.ds(index_ref[e], 1), :]
        table[side + 1 : side + 1 + tiles, 0:rows] = mask_ref[e].astype(jnp.float32)
        table_t[...] = table[...].T
        kept = jnp.where(iota((side, LANES), 1) < side, table_t[0:side, :], 0.0)
        kept = pltpu.roll(kept, LANES - half, axis=1)
        groups = [jnp.zeros((rows, LANES), jnp.float32) for _ in range(padded_depth // LANES)]
        for b in range(side):
            start = b * rows
            at = start % LANES
            row = jnp.broadcast_to(kept[b : b + 1, :], (rows, LANES))
            turned = pltpu.roll(row, at, axis=1, stride=1, stride_axis=0)
            inside = (lane >= at) & (lane < at + rows)
            groups[start // LANES] = jnp.where(inside, turned, groups[start // LANES])
        for g, value in enumerate(groups):
            taps[:, g * LANES : (g + 1) * LANES] = value
        image = images_ref[e]
        for b in range(side):
            move = b - half
            moved = pltpu.roll(image, (-move) % width, axis=1) if move else image
            inside = (column + move >= 0) & (column + move < width)
            shifted[b * rows : (b + 1) * rows, :] = jnp.where(inside, moved, 0.0)
        if padded_depth > depth:
            shifted[depth:, :] = jnp.zeros((padded_depth - depth, width), jnp.float32)
        difference = reference_ref[...] - dot(taps[...], shifted[...], ((1,), (0,)))
        for t in range(tiles):
            good = table_t[0:rows, side + 1 + t : side + 2 + t]
            piece = difference[:, t * LANES : (t + 1) * LANES] * good
            for r in range(0, rows, 8):
                first = (r * tiles + t) * local + e
                send[pl.ds(first, 8, stride=tiles * local), :] = piece[r : r + 8, :]

    sources = send.reshape(rows * tiles, local, LANES)
    def copy(source, target, semaphores, device):
        return pltpu.make_async_remote_copy(
            src_ref=source,
            dst_ref=target,
            send_sem=semaphores[0],
            recv_sem=semaphores[1],
            device_id={"ep": device},
            device_id_type=pl.DeviceIdType.MESH,
        )

    @pl.when(me != hub)
    def _():
        pl.semaphore_wait(barrier, 1)
        copy(sources, recv.at[:, me], (hub_send_sem, hub_sem), hub).start()

    @pl.when(me == hub)
    def _():
        pl.semaphore_wait(barrier, n - 1)
        for d in range(1, n):
            signal(ready_sem, lax.rem(me + d, n))
        recv[:, me] = sources[...]

    work[...] = jnp.zeros_like(work)
    epoch = iota((epochs, LANES), 0).astype(jnp.float32)
    template = iota((epochs, LANES), 1)
    onset = jnp.zeros((epochs, LANES), jnp.float32)
    for k in range(ntr):
        onset = jnp.where(template == k, onsets_ref[k].astype(jnp.float32), onset)
    delays = epoch - onset
    timescale = (template.astype(jnp.float32) + 1.0) * epochs / (2.0 * ntr)
    transient = jnp.where(delays >= 0.0, jnp.exp(-jnp.maximum(delays, 0.0) / timescale), 0.0)
    work[:, epochs : epochs + nsys] = systematics_ref[...]
    work[:, epochs + nsys : epochs + columns] = transient[:, 0:ntr]
    design = work[...]
    outer = dot(design, design, ((1,), (1,)))
    diagonal = iota((epochs, epochs), 0) == iota((epochs, epochs), 1)
    ridge = jnp.where(diagonal, cov_ridge, 0.0)
    work[:, 0:epochs] = fit_ridge * outer + ridge
    work[:, epochs + columns : 2 * epochs + columns] = ridge

    def drain(ref, semaphore):
        pltpu.make_async_copy(ref, ref, semaphore).wait()

    @pl.when(me != hub)
    def _():
        pl.semaphore_wait(ready_sem, 1)

    for d in range(n - 2):
        device = 2 + lax.rem(me + d, n - 2)

        @pl.when(me != device)
        def _():
            rows_of = sources.at[pl.ds(device * strips, strips)]
            copy(rows_of, pixels.at[:, me], (row_send_sem, row_sem), device).start()

    @pl.when(me > hub)
    def _():
        pixels[:, me] = sources[pl.ds(me * strips, strips)]

    @pl.when(me == hub)
    def _():
        drain(recv.at[:, 0 : n - 1], hub_sem)
        gathered = recv.reshape(pieces, epochs, LANES)
        step = min(pieces, 32)

        def gram(start):
            data = jnp.concatenate([gathered[start + i] for i in range(step)], axis=1)
            return dot(data, data, ((1,), (1,)))

        if step == pieces:
            partial_scatter = gram(0)
        else:
            partial_scatter = lax.fori_loop(
                0,
                pieces // step,
                lambda i, value: value + gram(i * step),
                jnp.zeros((epochs, epochs), jnp.float32),
            )
        share = epochs // pack
        if pack > 1:
            table[0:epochs, :] = jnp.zeros((epochs, LANES), jnp.float32)
            table[0:epochs, 0:epochs] = partial_scatter
            wide = table[0:epochs, :]
            packed = wide[0:share, :]
            for j in range(1, pack):
                packed = packed + pltpu.roll(
                    wide[j * share : (j + 1) * share, :], j * epochs, axis=1
                )
            total_ref[...] = packed
        else:
            total_ref[...] = partial_scatter
        for d in range(1, n):
            device = lax.rem(me + n - d, n)
            copy(total_ref, total_ref, (total_send_sem, total_sem), device).start()
        copy(recv.at[mate * strips : hub * strips], pixels, (row_send_sem, row_sem), mate).start()
        pixels[...] = recv[hub * strips : (hub + 1) * strips]

    @pl.when(me != hub)
    def _():
        drain(total_ref, total_sem)
        drain(sources, hub_send_sem)

    @pl.when(me == mate)
    def _():
        drain(pixels, row_sem)
        drain(pixels.at[:, 0 : n - 2], row_send_sem)

    @pl.when(me > hub)
    def _():
        drain(pixels.at[:, 0 : n - 1], row_sem)
        drain(pixels.at[:, 0 : n - 3], row_send_sem)

    @pl.when(me == hub)
    def _():
        drain(recv.at[0 : 2 * strips, 0 : n - 1], row_send_sem)
        drain(spare.at[0 : n - 1], total_send_sem)


def fit_kernel(npixels, pixels_ref, total_ref, base_ref, coefficients_ref, epoch_ref, work):
    columns, block, width = coefficients_ref.shape
    strips, n, local, _ = pixels_ref.shape
    epochs = n * local
    rows_of = pixels_ref.reshape(strips, epochs, LANES)
    data = jnp.concatenate([rows_of[i] for i in range(strips)], axis=1)
    pack = epochs // total_ref.shape[0]
    total = total_ref[...]
    if pack > 1:
        pieces = [total] + [
            pltpu.roll(total, LANES - j * epochs, axis=1) for j in range(1, pack)
        ]
        scatter = jnp.concatenate(pieces, axis=0)[:, 0:epochs]
    else:
        scatter = total

    covariance = scatter * (1.0 / npixels)
    work[...] = jnp.zeros_like(work)
    work[:, 0:epochs] = covariance
    work[:, epochs + columns : 2 * epochs + columns] = covariance
    system = work[...] + base_ref[...]
    lanes = system.shape[1]
    group = (8, lanes)
    strips = [system[i : i + 8, :] for i in range(0, epochs, 8)]
    index = iota(group, 0)

    def spread(value, row):
        return jnp.broadcast_to(value[row : row + 1, :], group)

    for home in range(epochs // 8):
        spans = [
            [jnp.broadcast_to(strip[:, k : k + 1], group) for strip in strips]
            for k in range(home * 8, home * 8 + 8)
        ]
        for row in range(0, 8, 2):
            lefts, rights = spans[row], spans[row + 1]
            a, b = spread(lefts[home], row), spread(rights[home], row)
            c, d = spread(lefts[home], row + 1), spread(rights[home], row + 1)
            inverse = 1.0 / (a * d - b * c)

            def step(values):
                first, second = spread(values[home], row), spread(values[home], row + 1)
                upper = (d * first - b * second) * inverse
                lower = (a * second - c * first) * inverse
                values = [
                    v - left * upper - right * lower
                    for v, left, right in zip(values, lefts, rights)
                ]
                values[home] = jnp.where(
                    index == row, upper, jnp.where(index == row + 1, lower, values[home])
                )
                return values

            spans = [step(span) if j > row + 1 else span for j, span in enumerate(spans)]
            strips = step(strips)
    system = jnp.concatenate(strips, axis=0)

    fitted = dot(system, data, ((0,), (0,)))[epochs : epochs + columns, :]
    for q in range(block):
        coefficients_ref[:, q, :] = fitted[:, q * width : (q + 1) * width]
    product = dot(scatter, system, ((1,), (0,))) * system
    work[0:1, :] = jnp.sum(product, axis=0, keepdims=True) * (1.0 / npixels)
    epoch_ref[...] = work[0, epochs + columns : 2 * epochs + columns]


HUB = 1


def ceil_to(value, unit):
    return -(-value // unit) * unit


def solution(mesh):
    n = mesh.shape["ep"]

    def shards(images, reference_image, kernels, kernel_index, tile_mask, systematics, onsets):
        local, rows, width = images.shape
        side = kernels.shape[1]
        tiles = width // LANES
        block = rows // n
        epochs = local * n
        columns = systematics.shape[1] + onsets.shape[0]
        pack = max(LANES // epochs, 1)
        share = epochs // pack
        part_lanes = max(LANES, epochs)
        vmem = pl.BlockSpec(memory_space=pltpu.VMEM)
        dma = pltpu.SemaphoreType.DMA
        f32 = jnp.float32
        flat_kernels = jnp.transpose(kernels, (1, 0, 2))
        flat_mask = jnp.transpose(tile_mask, (0, 2, 1))
        system_lanes = ceil_to(2 * epochs + columns, LANES)
        pieces = rows * tiles
        strips = block * tiles
        pixels, total, base = pl.pallas_call(
            functools.partial(exchange_kernel, n, HUB),
            out_shape=(
                jax.ShapeDtypeStruct((strips, n, local, LANES), f32),
                jax.ShapeDtypeStruct((share, part_lanes), f32),
                jax.ShapeDtypeStruct((epochs, system_lanes), f32),
            ),
            in_specs=[pl.BlockSpec(memory_space=pltpu.HBM)] * 7,
            out_specs=(vmem, vmem, vmem),
            scratch_shapes=[
                pltpu.VMEM(images.shape, f32),
                pltpu.VMEM(reference_image.shape, f32),
                pltpu.VMEM(flat_kernels.shape, f32),
                pltpu.SMEM(kernel_index.shape, jnp.int32),
                pltpu.VMEM(flat_mask.shape, jnp.int32),
                pltpu.VMEM(systematics.shape, f32),
                pltpu.SMEM(onsets.shape, jnp.int32),
                pltpu.VMEM((LANES, LANES), f32),
                pltpu.VMEM((LANES, LANES), f32),
                pltpu.VMEM((rows, ceil_to(side * rows, LANES)), f32),
                pltpu.VMEM((ceil_to(side * rows, LANES), width), f32),
                pltpu.VMEM((rows * tiles * local, LANES), f32),
                pltpu.VMEM((pieces, n, local, LANES), f32),
                pltpu.VMEM((n, share, part_lanes), f32),
                pltpu.SemaphoreType.DMA((7,)),
                pltpu.SemaphoreType.REGULAR,
                dma,
                dma,
                dma,
                dma,
                dma,
                dma,
            ],
            compiler_params=pltpu.CompilerParams(
                collective_id=0, has_side_effects=True, vmem_limit_bytes=VMEM_GRANT
            ),
        )(
            *(
                pltpu.with_memory_space_constraint(value, pltpu.HBM)
                for value in (
                    images,
                    reference_image,
                    flat_kernels,
                    kernel_index,
                    flat_mask,
                    systematics,
                    onsets,
                )
            )
        )
        return pl.pallas_call(
            functools.partial(fit_kernel, float(rows * width)),
            out_shape=(
                jax.ShapeDtypeStruct((columns, block, width), f32),
                jax.ShapeDtypeStruct((epochs,), f32),
            ),
            in_specs=[vmem, vmem, vmem],
            out_specs=(vmem, vmem),
            scratch_shapes=[pltpu.VMEM((epochs, system_lanes), f32)],
            compiler_params=pltpu.CompilerParams(vmem_limit_bytes=VMEM_GRANT),
        )(pixels, total, base)

    in_specs = (
        P(("field", "ep"), None, None),
        P("field", None),
        P(),
        P(("field", "ep")),
        P(("field", "ep"), None, None),
        P("field", None),
        P("field"),
    )
    out_specs = (P(None, ("field", "ep"), None), P("field"))
    return jax.shard_map(shards, mesh=mesh, in_specs=in_specs, out_specs=out_specs, check_vma=False)
```

```python
import functools

import jax
import jax.numpy as jnp
from jax import lax
from jax.experimental import pallas as pl
from jax.experimental.pallas import tpu as pltpu
from jax.sharding import PartitionSpec as P

cov_ridge = 0.5
fit_ridge = 1.0
LANES = 128
GROUP = 8
VMEM_GRANT = 24 * 2**20
HIGHEST = lax.Precision.HIGHEST


def dot(a, b, contract, precision=HIGHEST):
    return lax.dot_general(
        a, b, ((contract[0], contract[1]), ((), ())), precision=precision, preferred_element_type=jnp.float32
    )


def iota(shape, axis):
    return lax.broadcasted_iota(jnp.int32, shape, axis)


def cut(value, count):
    parts = []
    for _ in range(count - 1):
        parts.append(value.astype(jnp.bfloat16))
        value = value - parts[-1].astype(jnp.float32)
    return [*parts, value.astype(jnp.bfloat16)]


def plain_dot(a, b, contract):
    return lax.dot_general(
        a, b, ((contract[0], contract[1]), ((), ())), preferred_element_type=jnp.float32
    )


def turn(value, shift, stride):
    shift %= LANES
    if stride >= 0 and shift + 7 * stride <= LANES:
        return pltpu.roll(value, shift, axis=1, stride=stride, stride_axis=0)
    index = (iota(value.shape, 1) - shift - stride * iota(value.shape, 0)) & (LANES - 1)
    return jnp.take_along_axis(value, index, axis=1)


def exchange_kernel(
    n,
    hub,
    images_hbm,
    reference_hbm,
    kernels_hbm,
    index_hbm,
    mask_hbm,
    systematics_hbm,
    onsets_hbm,
    pixels,
    total_ref,
    work,
    images_ref,
    reference_ref,
    kernels_ref,
    index_ref,
    mask_ref,
    systematics_ref,
    onsets_ref,
    table,
    send,
    recv,
    spare,
    packed_ref,
    load_sem,
    ready_sem,
    row_sem,
    hub_sem,
    total_sem,
    hub_send_sem,
    row_send_sem,
    total_send_sem,
    mate_send_sem,
):
    local, rows, width = images_ref.shape
    side = kernels_hbm.shape[0]
    nk = kernels_hbm.shape[1]
    choices = kernels_ref.reshape(kernels_ref.shape[0] * nk, side)
    half = (side - 1) // 2
    tiles = width // LANES
    block = rows // n
    epochs = local * n
    nsys = systematics_ref.shape[1]
    ntr = onsets_ref.shape[0]
    columns = nsys + ntr
    pack = max(LANES // epochs, 1)
    me = lax.axis_index("ep")
    mate = hub - 1
    pieces = recv.shape[0]
    strips = block * tiles
    share = epochs // pack
    strip = iota((share, total_ref.shape[1]), 1) // epochs

    loads = [
        pltpu.make_async_copy(source, target, load_sem.at[i])
        for i, (source, target) in enumerate(
            (
                (index_hbm, index_ref),
                (kernels_hbm, kernels_ref.at[0:side]),
                (images_hbm, images_ref),
                (mask_hbm, mask_ref),
                (reference_hbm, reference_ref),
                (systematics_hbm, systematics_ref),
                (onsets_hbm, onsets_ref),
            )
        )
    ]
    for load in loads:
        load.start()

    def signal(semaphore, device):
        pl.semaphore_signal(
            semaphore, inc=1, device_id={"ep": device}, device_id_type=pl.DeviceIdType.MESH
        )

    barrier = pltpu.get_barrier_semaphore()

    @pl.when(me == hub)
    def _():
        for d in range(1, n):
            signal(barrier, lax.rem(me + d, n))

    @pl.when(me != hub)
    def _():
        signal(barrier, hub)

    table[...] = jnp.zeros_like(table)
    for load in loads:
        load.wait()

    steps = -(-side // GROUP)
    middle, offset = half // GROUP, half % GROUP
    depth = rows * GROUP
    lane = iota((8, LANES), 1)
    sublane = iota((8, LANES), 0)
    place = lane + sublane - offset
    good = {}
    for e in range(local):
        at = LANES - (e + 1) * 8
        table[at : at + tiles, 0:rows] = mask_ref[e].astype(jnp.float32)
        for t in range(tiles):
            row = jnp.broadcast_to(table[at + t : at + t + 1, :], (8, LANES))
            for r in range(0, rows, 8):
                good[e, t, r] = jnp.take_along_axis(row, sublane + r, axis=1)
    for e in range(local):
        banks = -(-side // 8)
        turned = []
        for g in range(banks):
            table[8 * g : 8 * g + 8, 0:side] = choices[pl.ds(index_ref[e] + 8 * g * nk, 8, stride=nk), :]
            turned.append(
                turn(table[8 * g : 8 * g + 8, :], 8 * g * GROUP, GROUP)
            )
        pages = -(-(GROUP * side + side) // LANES)
        bands = []
        for m in range(steps):
            flat = []
            for page in range(pages):
                total = jnp.zeros((8, LANES), jnp.float32)
                for g in range(banks):
                    low = GROUP * (8 * g + m) - page * LANES
                    if low + 8 * GROUP <= 0 or low >= LANES:
                        continue
                    away = lane - GROUP * sublane - low
                    inside = (away >= 0) & (away < GROUP) & (sublane < side - 8 * g)
                    total = total + jnp.where(inside, turned[g], 0.0)
                flat.append(jnp.broadcast_to(jnp.sum(total, axis=0, keepdims=True), (8, LANES)))
            for h in range(rows // 8):
                pieces_of = []
                for start in range(0, depth, LANES):
                    base = start + GROUP * (half + m - 8 * h)
                    spot = lane + base - GROUP * sublane
                    value = jnp.zeros((8, LANES), jnp.float32)
                    for page in range(pages):
                        if base + LANES <= page * LANES or base - 7 * GROUP >= (page + 1) * LANES:
                            continue
                        moved = turn(flat[page], -base, GROUP)
                        inside = (spot >= page * LANES) & (spot < (page + 1) * LANES)
                        value = jnp.where(inside, moved, value)
                    pieces_of.append(value)
                bands.append(jnp.concatenate(pieces_of, axis=1))
        spread_rows = []
        for r in range(rows):
            moved = [
                turn(
                    jnp.broadcast_to(
                        images_ref[e, r : r + 1, t * LANES : (t + 1) * LANES], (8, LANES)
                    ),
                    offset,
                    -1,
                )
                for t in range(tiles)
            ]
            moved.append(None)
            parts_of = []
            for t in range(tiles + 1):
                value = jnp.zeros((8, LANES), jnp.float32) if moved[t] is None else moved[t]
                before, after = moved[t - 1], moved[(t + 1) % (tiles + 1)]
                value = jnp.where(place < 0, 0.0 if before is None else before, value)
                value = jnp.where(place >= LANES, 0.0 if after is None else after, value)
                parts_of.append(value)
            spread_rows.append(jnp.concatenate(parts_of, axis=1))
        response = dot(
            jnp.concatenate(bands, axis=0),
            jnp.concatenate(spread_rows, axis=0),
            ((1,), (0,)),
            lax.Precision.HIGH,
        )
        span = width + LANES
        model = response[middle * rows : (middle + 1) * rows, 0:width]
        for m in range(steps):
            if m != middle:
                part = response[m * rows : (m + 1) * rows, :]
                model = model + pltpu.roll(part, (-GROUP * (m - middle)) % span, axis=1)[:, 0:width]
        difference = reference_ref[...] - model
        for t in range(tiles):
            for r in range(0, rows, 8):
                first = (r * tiles + t) * local + e
                piece = difference[r : r + 8, t * LANES : (t + 1) * LANES]
                send[pl.ds(first, 8, stride=tiles * local), :] = piece * good[e, t, r]

    sources = send.reshape(rows * tiles, local, LANES)
    def copy(source, target, semaphores, device):
        return pltpu.make_async_remote_copy(
            src_ref=source,
            dst_ref=target,
            send_sem=semaphores[0],
            recv_sem=semaphores[1],
            device_id={"ep": device},
            device_id_type=pl.DeviceIdType.MESH,
        )

    @pl.when(me != hub)
    def _():
        pl.semaphore_wait(barrier, 1)
        copy(sources, recv.at[:, me], (hub_send_sem, hub_sem), hub).start()

    @pl.when(me == hub)
    def _():
        pl.semaphore_wait(barrier, n - 1)
        for d in range(1, n):
            signal(ready_sem, lax.rem(me + d, n))
        recv[:, me] = sources[...]

    work[...] = jnp.zeros_like(work)
    epoch = iota((epochs, LANES), 0).astype(jnp.float32)
    template = iota((epochs, LANES), 1)
    onset = jnp.zeros((epochs, LANES), jnp.float32)
    for k in range(ntr):
        onset = jnp.where(template == k, onsets_ref[k].astype(jnp.float32), onset)
    delays = epoch - onset
    timescale = (template.astype(jnp.float32) + 1.0) * epochs / (2.0 * ntr)
    transient = jnp.where(delays >= 0.0, jnp.exp(-jnp.maximum(delays, 0.0) / timescale), 0.0)
    work[:, epochs : epochs + nsys] = systematics_ref[...]
    work[:, epochs + nsys : epochs + columns] = transient[:, 0:ntr]
    design = work[...]
    outer = dot(design, design, ((1,), (1,)))
    diagonal = iota((epochs, epochs), 0) == iota((epochs, epochs), 1)
    ridge = jnp.where(diagonal, cov_ridge, 0.0)
    lanes = work.shape[1]
    work[:, 0:epochs] = ridge
    work[:, lanes - epochs : lanes] = fit_ridge * outer + ridge

    def drain(ref, semaphore):
        pltpu.make_async_copy(ref, ref, semaphore).wait()

    @pl.when(me != hub)
    def _():
        pl.semaphore_wait(ready_sem, 1)

    for d in range(n - 2):
        device = 2 + lax.rem(me + d, n - 2)

        @pl.when(me != device)
        def _():
            rows_of = sources.at[pl.ds(device * strips, strips)]
            copy(rows_of, pixels.at[:, me], (row_send_sem, row_sem), device).start()

    @pl.when(me > hub)
    def _():
        pixels[:, me] = sources[pl.ds(me * strips, strips)]

    @pl.when(me == hub)
    def _():
        drain(recv.at[:, 0 : n - 1], hub_sem)
        gathered = recv.reshape(pieces, epochs, LANES)
        step = min(pieces, 32)

        def gram(start):
            data = jnp.concatenate([gathered[start + i] for i in range(step)], axis=1)
            both = jnp.concatenate(cut(data, 2), axis=0)
            square = plain_dot(both, both, ((1,), (1,)))
            return square[0:epochs] + square[epochs : 2 * epochs]

        if step == pieces:
            square = gram(0)
        else:
            square = lax.fori_loop(
                0,
                pieces // step,
                lambda i, value: value + gram(i * step),
                jnp.zeros((epochs, 2 * epochs), jnp.float32),
            )
        if pack > 1:
            table[0:epochs, 2 * epochs :] = jnp.zeros((epochs, LANES - 2 * epochs), jnp.float32)
            table[0:epochs, 0 : 2 * epochs] = square
            wide = table[0:epochs, :]
            total = wide
            for j in range(1, pack):
                total = total + pltpu.roll(wide, j * epochs, axis=1)
            total_ref[...] = total
            packed = total[0:share, :]
            for j in range(1, pack):
                packed = jnp.where(strip == j, total[j * share : (j + 1) * share, :], packed)
            packed_ref[...] = packed
        else:
            total_ref[...] = square[:, 0:epochs] + square[:, epochs : 2 * epochs]
        for d in range(1, n):
            device = lax.rem(me + n - d, n)
            if d == 1 and pack > 1:
                copy(total_ref, total_ref, (mate_send_sem, total_sem), device).start()
            elif pack > 1:
                copy(packed_ref, packed_ref, (total_send_sem, total_sem), device).start()
            else:
                copy(total_ref, total_ref, (total_send_sem, total_sem), device).start()
        copy(recv.at[mate * strips : hub * strips], pixels, (row_send_sem, row_sem), mate).start()
        pixels[...] = recv[hub * strips : (hub + 1) * strips]

    @pl.when(me == mate)
    def _():
        drain(total_ref, total_sem)
        drain(sources, hub_send_sem)
        drain(pixels, row_sem)
        drain(pixels.at[:, 0 : n - 2], row_send_sem)

    @pl.when(me > hub)
    def _():
        if pack > 1:
            drain(packed_ref, total_sem)
            packed = packed_ref[...]
            for j in range(pack):
                one = jnp.where(strip == j, packed, 0.0)
                total = one
                for k in range(1, pack):
                    total = total + pltpu.roll(one, k * epochs, axis=1)
                total_ref[j * share : (j + 1) * share, :] = total
        else:
            drain(total_ref, total_sem)
        drain(sources, hub_send_sem)
        drain(pixels.at[:, 0 : n - 1], row_sem)
        drain(pixels.at[:, 0 : n - 3], row_send_sem)

    @pl.when(me == hub)
    def _():
        drain(recv.at[0 : 2 * strips, 0 : n - 1], row_send_sem)
        if pack > 1:
            drain(spare.at[0 : n - 2], total_send_sem)
            drain(total_ref, mate_send_sem)
        else:
            drain(spare.at[0 : n - 1], total_send_sem)


def split_dot(a, b):
    high, middle, low = cut(a, 3)
    left = jnp.concatenate([high, high, middle, high, middle, low], axis=0)
    high, middle, low = cut(b, 3)
    right = jnp.concatenate([high, middle, high, low, middle, high], axis=0)
    return plain_dot(left, right, ((0,), (0,)))


def fit_kernel(npixels, pixels_ref, total_ref, base_ref, coefficients_ref, epoch_ref, work):
    columns, block, width = coefficients_ref.shape
    strips, n, local, _ = pixels_ref.shape
    epochs = n * local
    rows_of = pixels_ref.reshape(strips, epochs, LANES)
    data = jnp.concatenate([rows_of[i] for i in range(strips)], axis=1)
    total = total_ref[...]
    lanes = base_ref.shape[1]
    lane = iota((epochs, lanes), 1)
    covariance = jnp.concatenate([total] * (lanes // total.shape[1]), axis=1) * (1.0 / npixels)
    ends = (lane < epochs) | (lane >= lanes - epochs)
    system = base_ref[...] + jnp.where(ends, covariance, 0.0)
    group = (8, lanes)
    strips = [system[i : i + 8, :] for i in range(0, epochs, 8)]
    index = iota(group, 0)

    def column(value, at):
        tile = at // LANES * LANES
        value = value[:, tile : tile + LANES]
        value = jnp.take_along_axis(value, jnp.full((8, LANES), at - tile, jnp.int32), axis=1)
        return jnp.concatenate([value] * (lanes // LANES), axis=1)

    def spread(value, row):
        return jnp.broadcast_to(value[row : row + 1, :], group)

    for home in range(epochs // 8):
        first_lane = lanes - epochs + home * 8
        spans = [column(strips[home], first_lane + k) for k in range(8)]
        others = [i for i in range(epochs // 8) if i != home]
        factors = {i: [column(strips[i], first_lane + k) for k in range(8)] for i in others}
        value = strips[home]
        for row in range(0, 8, 2):
            left, right = spans[row], spans[row + 1]
            a, b = spread(left, row), spread(right, row)
            c, d = spread(left, row + 1), spread(right, row + 1)
            inverse = 1.0 / (a * d - b * c)

            def step(value):
                first, second = spread(value, row), spread(value, row + 1)
                upper = (d * first - b * second) * inverse
                lower = (a * second - c * first) * inverse
                value = value - left * upper - right * lower
                return jnp.where(index == row, upper, jnp.where(index == row + 1, lower, value))

            spans = [step(span) if j > row + 1 else span for j, span in enumerate(spans)]
            value = step(value)
        strips[home] = value
        pivots = [spread(value, k) for k in range(8)]
        for i in others:
            terms = [factor * pivot for factor, pivot in zip(factors[i], pivots)]
            while len(terms) > 1:
                terms = [p + q for p, q in zip(terms[0::2], terms[1::2])]
            strips[i] = strips[i] - terms[0]
    system = jnp.concatenate(strips, axis=0)

    solved = system[:, 0:LANES] if epochs < LANES else system[:, 0:epochs]
    scatter = total[:, 0:epochs]
    if epochs * 4 == total.shape[1]:
        parts = [part.astype(jnp.float32) for part in cut(total, 3)]
        high, middle, low = parts
        block_of = iota(total.shape, 1) // epochs
        front = jnp.where(block_of == 2, middle, high)
        back = jnp.where(block_of == 0, middle, jnp.where(block_of == 1, low, 0.0))
        left = jnp.concatenate([front, back], axis=1).astype(jnp.bfloat16)
        high, middle, low = cut(solved, 3)
        right = jnp.concatenate([high, middle, high, low, middle, high, high, high], axis=0)
        product = plain_dot(left, right, ((1,), (0,))) * solved
    else:
        product = dot(scatter, solved, ((1,), (0,))) * solved
    epoch_ref[...] = (jnp.sum(product, axis=0, keepdims=True) * (1.0 / npixels))[0, 0:epochs]

    if 6 * epochs <= 256:
        fitted = split_dot(system, data)
    else:
        fitted = dot(system, data, ((0,), (0,)))
    fitted = fitted[epochs : epochs + columns, :]
    for q in range(block):
        coefficients_ref[:, q, :] = fitted[:, q * width : (q + 1) * width]


HUB = 1


def ceil_to(value, unit):
    return -(-value // unit) * unit


def solution(mesh):
    n = mesh.shape["ep"]

    def shards(images, reference_image, kernels, kernel_index, tile_mask, systematics, onsets):
        local, rows, width = images.shape
        side = kernels.shape[1]
        tiles = width // LANES
        block = rows // n
        epochs = local * n
        columns = systematics.shape[1] + onsets.shape[0]
        pack = max(LANES // epochs, 1)
        share = epochs // pack
        part_lanes = max(LANES, epochs)
        vmem = pl.BlockSpec(memory_space=pltpu.VMEM)
        dma = pltpu.SemaphoreType.DMA
        f32 = jnp.float32
        flat_kernels = jnp.transpose(kernels, (1, 0, 2))
        flat_mask = jnp.transpose(tile_mask, (0, 2, 1))
        system_lanes = ceil_to(2 * epochs + columns, LANES)
        pieces = rows * tiles
        strips = block * tiles
        pixels, total, base = pl.pallas_call(
            functools.partial(exchange_kernel, n, HUB),
            out_shape=(
                jax.ShapeDtypeStruct((strips, n, local, LANES), f32),
                jax.ShapeDtypeStruct((epochs, part_lanes), f32),
                jax.ShapeDtypeStruct((epochs, system_lanes), f32),
            ),
            in_specs=[pl.BlockSpec(memory_space=pltpu.HBM)] * 7,
            out_specs=(vmem, vmem, vmem),
            scratch_shapes=[
                pltpu.VMEM(images.shape, f32),
                pltpu.VMEM(reference_image.shape, f32),
                pltpu.VMEM((ceil_to(side, 8), *flat_kernels.shape[1:]), f32),
                pltpu.SMEM(kernel_index.shape, jnp.int32),
                pltpu.VMEM(flat_mask.shape, jnp.int32),
                pltpu.VMEM(systematics.shape, f32),
                pltpu.SMEM(onsets.shape, jnp.int32),
                pltpu.VMEM((LANES, LANES), f32),
                pltpu.VMEM((rows * tiles * local, LANES), f32),
                pltpu.VMEM((pieces, n, local, LANES), f32),
                pltpu.VMEM((n, share, part_lanes), f32),
                pltpu.VMEM((share, part_lanes), f32),
                pltpu.SemaphoreType.DMA((7,)),
                pltpu.SemaphoreType.REGULAR,
                dma,
                dma,
                dma,
                dma,
                dma,
                dma,
                dma,
            ],
            compiler_params=pltpu.CompilerParams(
                collective_id=0, has_side_effects=True, vmem_limit_bytes=VMEM_GRANT
            ),
        )(
            *(
                pltpu.with_memory_space_constraint(value, pltpu.HBM)
                for value in (
                    images,
                    reference_image,
                    flat_kernels,
                    kernel_index,
                    flat_mask,
                    systematics,
                    onsets,
                )
            )
        )
        return pl.pallas_call(
            functools.partial(fit_kernel, float(rows * width)),
            out_shape=(
                jax.ShapeDtypeStruct((columns, block, width), f32),
                jax.ShapeDtypeStruct((epochs,), f32),
            ),
            in_specs=[vmem, vmem, vmem],
            out_specs=(vmem, vmem),
            scratch_shapes=[pltpu.VMEM((epochs, system_lanes), f32)],
            compiler_params=pltpu.CompilerParams(vmem_limit_bytes=VMEM_GRANT),
        )(pixels, total, base)

    in_specs = (
        P(("field", "ep"), None, None),
        P("field", None),
        P(),
        P(("field", "ep")),
        P(("field", "ep"), None, None),
        P("field", None),
        P("field"),
    )
    out_specs = (P(None, ("field", "ep"), None), P("field"))
    return jax.shard_map(shards, mesh=mesh, in_specs=in_specs, out_specs=out_specs, check_vma=False)
```

```python
import functools

import jax
import jax.numpy as jnp
from jax import lax
from jax.experimental import pallas as pl
from jax.experimental.pallas import tpu as pltpu
from jax.sharding import PartitionSpec as P

cov_ridge = 0.5
fit_ridge = 1.0
LANES = 128
GROUP = 8
VMEM_GRANT = 24 * 2**20
HIGHEST = lax.Precision.HIGHEST


def dot(a, b, contract, precision=HIGHEST):
    return lax.dot_general(
        a, b, ((contract[0], contract[1]), ((), ())), precision=precision, preferred_element_type=jnp.float32
    )


def iota(shape, axis):
    return lax.broadcasted_iota(jnp.int32, shape, axis)


def cut(value, count):
    parts = []
    for _ in range(count - 1):
        parts.append(value.astype(jnp.bfloat16))
        value = value - parts[-1].astype(jnp.float32)
    return [*parts, value.astype(jnp.bfloat16)]


def plain_dot(a, b, contract):
    return lax.dot_general(
        a, b, ((contract[0], contract[1]), ((), ())), preferred_element_type=jnp.float32
    )


def turn(value, shift, stride):
    shift %= LANES
    if stride >= 0 and shift + 7 * stride <= LANES:
        return pltpu.roll(value, shift, axis=1, stride=stride, stride_axis=0)
    index = (iota(value.shape, 1) - shift - stride * iota(value.shape, 0)) & (LANES - 1)
    return jnp.take_along_axis(value, index, axis=1)


def solve(total, base, npixels):
    epochs, lanes = base.shape
    lane = iota((epochs, lanes), 1)
    covariance = jnp.concatenate([total] * (lanes // total.shape[1]), axis=1) * (1.0 / npixels)
    ends = (lane < epochs) | (lane >= lanes - epochs)
    system = base + jnp.where(ends, covariance, 0.0)
    group = (8, lanes)
    strips = [system[i : i + 8, :] for i in range(0, epochs, 8)]
    index = iota(group, 0)

    def column(value, at):
        tile = at // LANES * LANES
        value = value[:, tile : tile + LANES]
        value = jnp.take_along_axis(value, jnp.full((8, LANES), at - tile, jnp.int32), axis=1)
        return jnp.concatenate([value] * (lanes // LANES), axis=1)

    def spread(value, row):
        return jnp.broadcast_to(value[row : row + 1, :], group)

    def total_of(terms):
        while len(terms) > 1:
            terms = [p + q for p, q in zip(terms[0::2], terms[1::2])]
        return terms[0]

    size = 2 if epochs % 16 == 0 else 1
    for start in range(0, epochs // 8, size):
        home = range(start, start + size)
        order = [i for i in range(epochs // 8) if i not in home]
        at = lanes - epochs + start * 8
        spans = [[column(strips[i], at + k) for i in home] for k in range(8 * size)]
        factors = [[column(strips[i], at + k) for k in range(8 * size)] for i in order]
        values = [strips[i] for i in home]
        for first_row in range(0, 8 * size, 2):
            owner, row = divmod(first_row, 8)
            lefts, rights = spans[first_row], spans[first_row + 1]
            a, b = spread(lefts[owner], row), spread(rights[owner], row)
            c, d = spread(lefts[owner], row + 1), spread(rights[owner], row + 1)
            inverse = 1.0 / (a * d - b * c)
            upper, lower = index == row, index == row + 1
            pair = upper | lower
            weights = []
            for i in range(size):
                one, two = rights[i] * c - lefts[i] * d, lefts[i] * b - rights[i] * a
                if i == owner:
                    one = jnp.where(upper, d, jnp.where(lower, -c, one))
                    two = jnp.where(upper, -b, jnp.where(lower, a, two))
                weights.append((one * inverse, two * inverse))

            def step(values):
                first, second = spread(values[owner], row), spread(values[owner], row + 1)
                return [
                    (jnp.where(pair, 0.0, value) if i == owner else value)
                    + weights[i][0] * first
                    + weights[i][1] * second
                    for i, value in enumerate(values)
                ]

            spans = [step(span) if j > first_row + 1 else span for j, span in enumerate(spans)]
            values = step(values)
        pivots = [spread(values[k // 8], k % 8) for k in range(8 * size)]
        for i, factor in zip(order, factors):
            strips[i] = strips[i] - total_of([p * q for p, q in zip(factor, pivots)])
        for i, value in zip(home, values):
            strips[i] = value
    return jnp.concatenate(strips, axis=0)


def exchange_kernel(
    n,
    hub,
    images_hbm,
    reference_hbm,
    kernels_hbm,
    index_hbm,
    mask_hbm,
    systematics_hbm,
    onsets_hbm,
    pixels,
    total_ref,
    system_ref,
    images_ref,
    reference_ref,
    kernels_ref,
    index_ref,
    mask_ref,
    systematics_ref,
    onsets_ref,
    table,
    work,
    send,
    recv,
    spare,
    packed_ref,
    load_sem,
    ready_sem,
    row_sem,
    hub_sem,
    total_sem,
    hub_send_sem,
    row_send_sem,
    total_send_sem,
    mate_send_sem,
):
    local, rows, width = images_ref.shape
    side = kernels_hbm.shape[0]
    nk = kernels_hbm.shape[1]
    choices = kernels_ref.reshape(kernels_ref.shape[0] * nk, side)
    half = (side - 1) // 2
    tiles = width // LANES
    block = rows // n
    epochs = local * n
    nsys = systematics_ref.shape[1]
    ntr = onsets_ref.shape[0]
    columns = nsys + ntr
    pack = max(LANES // epochs, 1)
    me = lax.axis_index("ep")
    mate = hub - 1
    pieces = recv.shape[0]
    strips = block * tiles
    share = epochs // pack
    strip = iota((share, total_ref.shape[1]), 1) // epochs

    loads = [
        pltpu.make_async_copy(source, target, load_sem.at[i])
        for i, (source, target) in enumerate(
            (
                (index_hbm, index_ref),
                (kernels_hbm, kernels_ref.at[0:side]),
                (images_hbm, images_ref),
                (mask_hbm, mask_ref),
                (reference_hbm, reference_ref),
                (systematics_hbm, systematics_ref),
                (onsets_hbm, onsets_ref),
            )
        )
    ]
    for load in loads:
        load.start()

    def signal(semaphore, device):
        pl.semaphore_signal(
            semaphore, inc=1, device_id={"ep": device}, device_id_type=pl.DeviceIdType.MESH
        )

    barrier = pltpu.get_barrier_semaphore()

    @pl.when(me == hub)
    def _():
        for d in range(1, n):
            signal(barrier, lax.rem(me + d, n))

    @pl.when(me != hub)
    def _():
        signal(barrier, hub)

    table[...] = jnp.zeros_like(table)
    for load in loads:
        load.wait()

    steps = -(-side // GROUP)
    middle, offset = half // GROUP, half % GROUP
    depth = rows * GROUP
    lane = iota((8, LANES), 1)
    sublane = iota((8, LANES), 0)
    place = lane + sublane - offset
    banks = -(-side // 8)
    pages = -(-(GROUP * side + side) // LANES)
    turned = []
    for e in range(local):
        at = e * 8 * banks
        for g in range(banks):
            table[at + 8 * g : at + 8 * g + 8, 0:side] = choices[
                pl.ds(index_ref[e] + 8 * g * nk, 8, stride=nk), :
            ]
    for e in range(local):
        at = e * 8 * banks
        turned.append(
            [
                turn(table[at + 8 * g : at + 8 * g + 8, :], 8 * g * GROUP, GROUP)
                for g in range(banks)
            ]
        )
    windows = {}
    for m in range(steps):
        for page in range(pages):
            for g in range(banks):
                low = GROUP * (8 * g + m) - page * LANES
                if low + 8 * GROUP > 0 and low < LANES:
                    away = lane - GROUP * sublane - low
                    inside = (away >= 0) & (away < GROUP) & (sublane < side - 8 * g)
                    windows[m, page, g] = inside
    flats = {}
    for m in range(steps):
        for e in range(local):
            for page in range(pages):
                total = jnp.zeros((8, LANES), jnp.float32)
                for g in range(banks):
                    if (m, page, g) in windows:
                        total = total + jnp.where(windows[m, page, g], turned[e][g], 0.0)
                total = jnp.sum(total, axis=0, keepdims=True)
                flats[e, m, page] = jnp.broadcast_to(total, (8, LANES))
    bands = [[] for _ in range(local)]
    for m in range(steps):
        for h in range(rows // 8):
            for e in range(local):
                pieces_of = []
                for start in range(0, depth, LANES):
                    base = start + GROUP * (half + m - 8 * h)
                    spot = lane + base - GROUP * sublane
                    value = jnp.zeros((8, LANES), jnp.float32)
                    for page in range(pages):
                        if base + LANES <= page * LANES or base - 7 * GROUP >= (page + 1) * LANES:
                            continue
                        moved = turn(flats[e, m, page], -base, GROUP)
                        inside = (spot >= page * LANES) & (spot < (page + 1) * LANES)
                        value = jnp.where(inside, moved, value)
                    pieces_of.append(value)
                bands[e].append(jnp.concatenate(pieces_of, axis=1))
    good = {}
    for e in range(local):
        at = table.shape[0] - (e + 1) * 8
        table[at : at + tiles, 0:rows] = mask_ref[e].astype(jnp.float32)
        for t in range(tiles):
            row = jnp.broadcast_to(table[at + t : at + t + 1, :], (8, LANES))
            for r in range(0, rows, 8):
                good[e, t, r] = jnp.take_along_axis(row, sublane + r, axis=1)
    for e in range(local):
        spread_rows = []
        for r in range(rows):
            moved = [
                turn(
                    jnp.broadcast_to(
                        images_ref[e, r : r + 1, t * LANES : (t + 1) * LANES], (8, LANES)
                    ),
                    offset,
                    -1,
                )
                for t in range(tiles)
            ]
            moved.append(None)
            parts_of = []
            for t in range(tiles + 1):
                value = jnp.zeros((8, LANES), jnp.float32) if moved[t] is None else moved[t]
                before, after = moved[t - 1], moved[(t + 1) % (tiles + 1)]
                value = jnp.where(place < 0, 0.0 if before is None else before, value)
                value = jnp.where(place >= LANES, 0.0 if after is None else after, value)
                parts_of.append(value)
            spread_rows.append(jnp.concatenate(parts_of, axis=1))
        response = dot(
            jnp.concatenate(bands[e], axis=0),
            jnp.concatenate(spread_rows, axis=0),
            ((1,), (0,)),
            lax.Precision.HIGH,
        )
        span = width + LANES
        model = response[middle * rows : (middle + 1) * rows, 0:width]
        for m in range(steps):
            if m != middle:
                part = response[m * rows : (m + 1) * rows, :]
                model = model + pltpu.roll(part, (-GROUP * (m - middle)) % span, axis=1)[:, 0:width]
        difference = reference_ref[...] - model
        for t in range(tiles):
            for r in range(0, rows, 8):
                first = (r * tiles + t) * local + e
                piece = difference[r : r + 8, t * LANES : (t + 1) * LANES]
                send[pl.ds(first, 8, stride=tiles * local), :] = piece * good[e, t, r]

    sources = send.reshape(rows * tiles, local, LANES)
    def copy(source, target, semaphores, device):
        return pltpu.make_async_remote_copy(
            src_ref=source,
            dst_ref=target,
            send_sem=semaphores[0],
            recv_sem=semaphores[1],
            device_id={"ep": device},
            device_id_type=pl.DeviceIdType.MESH,
        )

    @pl.when(me != hub)
    def _():
        pl.semaphore_wait(barrier, 1)
        copy(sources, recv.at[:, me], (hub_send_sem, hub_sem), hub).start()

    @pl.when(me == hub)
    def _():
        pl.semaphore_wait(barrier, n - 1)
        for d in range(1, n):
            signal(ready_sem, lax.rem(me + d, n))
        recv[:, me] = sources[...]

    work[...] = jnp.zeros_like(work)
    epoch = iota((epochs, LANES), 0).astype(jnp.float32)
    template = iota((epochs, LANES), 1)
    onset = jnp.zeros((epochs, LANES), jnp.float32)
    for k in range(ntr):
        onset = jnp.where(template == k, onsets_ref[k].astype(jnp.float32), onset)
    delays = epoch - onset
    timescale = (template.astype(jnp.float32) + 1.0) * epochs / (2.0 * ntr)
    transient = jnp.where(delays >= 0.0, jnp.exp(-jnp.maximum(delays, 0.0) / timescale), 0.0)
    work[:, epochs : epochs + nsys] = systematics_ref[...]
    work[:, epochs + nsys : epochs + columns] = transient[:, 0:ntr]
    design = work[...]
    outer = dot(design, design, ((1,), (1,)))
    diagonal = iota((epochs, epochs), 0) == iota((epochs, epochs), 1)
    ridge = jnp.where(diagonal, cov_ridge, 0.0)
    lanes = work.shape[1]
    work[:, 0:epochs] = ridge
    work[:, lanes - epochs : lanes] = fit_ridge * outer + ridge

    def drain(ref, semaphore):
        pltpu.make_async_copy(ref, ref, semaphore).wait()

    @pl.when(me != hub)
    def _():
        pl.semaphore_wait(ready_sem, 1)

    for d in range(n - 2):
        device = 2 + lax.rem(me + d, n - 2)

        @pl.when(me != device)
        def _():
            rows_of = sources.at[pl.ds(device * strips, strips)]
            copy(rows_of, pixels.at[:, me], (row_send_sem, row_sem), device).start()

    @pl.when(me > hub)
    def _():
        pixels[:, me] = sources[pl.ds(me * strips, strips)]

    @pl.when(me == hub)
    def _():
        drain(recv.at[:, 0 : n - 1], hub_sem)
        copy(recv.at[mate * strips : hub * strips], pixels, (row_send_sem, row_sem), mate).start()
        gathered = recv.reshape(pieces, epochs, LANES)
        step = min(pieces, 32)

        def gram(start):
            data = jnp.concatenate([gathered[start + i] for i in range(step)], axis=1)
            both = jnp.concatenate(cut(data, 2), axis=0)
            square = plain_dot(both, both, ((1,), (1,)))
            return square[0:epochs] + square[epochs : 2 * epochs]

        if step == pieces:
            square = gram(0)
        else:
            square = lax.fori_loop(
                0,
                pieces // step,
                lambda i, value: value + gram(i * step),
                jnp.zeros((epochs, 2 * epochs), jnp.float32),
            )
        if pack > 1:
            table[0:epochs, 2 * epochs :] = jnp.zeros((epochs, LANES - 2 * epochs), jnp.float32)
            table[0:epochs, 0 : 2 * epochs] = square
            wide = table[0:epochs, :]
            total = wide
            for j in range(1, pack):
                total = total + pltpu.roll(wide, j * epochs, axis=1)
            total_ref[...] = total
            packed = total[0:share, :]
            for j in range(1, pack):
                packed = jnp.where(strip == j, total[j * share : (j + 1) * share, :], packed)
            packed_ref[...] = packed
        else:
            total_ref[...] = square[:, 0:epochs] + square[:, epochs : 2 * epochs]
        for d in range(1, n):
            device = lax.rem(me + n - d, n)
            if d == 1 and pack > 1:
                copy(total_ref, total_ref, (mate_send_sem, total_sem), device).start()
            elif pack > 1:
                copy(packed_ref, packed_ref, (total_send_sem, total_sem), device).start()
            else:
                copy(total_ref, total_ref, (total_send_sem, total_sem), device).start()
        pixels[...] = recv[hub * strips : (hub + 1) * strips]

    @pl.when(me == mate)
    def _():
        drain(total_ref, total_sem)

    @pl.when(me > hub)
    def _():
        if pack > 1:
            drain(packed_ref, total_sem)
            packed = packed_ref[...]
            for j in range(pack):
                one = jnp.where(strip == j, packed, 0.0)
                total = one
                for k in range(1, pack):
                    total = total + pltpu.roll(one, k * epochs, axis=1)
                total_ref[j * share : (j + 1) * share, :] = total
        else:
            drain(total_ref, total_sem)

    system_ref[...] = solve(total_ref[...], work[...], float(rows * width))

    @pl.when(me == mate)
    def _():
        drain(sources, hub_send_sem)
        drain(pixels, row_sem)
        drain(pixels.at[:, 0 : n - 2], row_send_sem)

    @pl.when(me > hub)
    def _():
        drain(sources, hub_send_sem)
        drain(pixels.at[:, 0 : n - 1], row_sem)
        drain(pixels.at[:, 0 : n - 3], row_send_sem)

    @pl.when(me == hub)
    def _():
        drain(recv.at[0 : 2 * strips, 0 : n - 1], row_send_sem)
        if pack > 1:
            drain(spare.at[0 : n - 2], total_send_sem)
            drain(total_ref, mate_send_sem)
        else:
            drain(spare.at[0 : n - 1], total_send_sem)


def split_dot(a, b):
    high, middle, low = cut(a, 3)
    left = jnp.concatenate([high, high, middle, high, middle, low], axis=0)
    high, middle, low = cut(b, 3)
    right = jnp.concatenate([high, middle, high, low, middle, high], axis=0)
    return plain_dot(left, right, ((0,), (0,)))


def fit_kernel(npixels, pixels_ref, total_ref, system_ref, coefficients_ref, epoch_ref):
    columns, block, width = coefficients_ref.shape
    strips, n, local, _ = pixels_ref.shape
    epochs = n * local
    rows_of = pixels_ref.reshape(strips, epochs, LANES)
    data = jnp.concatenate([rows_of[i] for i in range(strips)], axis=1)
    total = total_ref[...]
    system = system_ref[...]

    solved = system[:, 0:LANES] if epochs < LANES else system[:, 0:epochs]
    scatter = total[:, 0:epochs]
    if epochs * 4 == total.shape[1]:
        parts = [part.astype(jnp.float32) for part in cut(total, 3)]
        high, middle, low = parts
        block_of = iota(total.shape, 1) // epochs
        front = jnp.where(block_of == 2, middle, high)
        back = jnp.where(block_of == 0, middle, jnp.where(block_of == 1, low, 0.0))
        left = jnp.concatenate([front, back], axis=1).astype(jnp.bfloat16)
        high, middle, low = cut(solved, 3)
        right = jnp.concatenate([high, middle, high, low, middle, high, high, high], axis=0)
        product = plain_dot(left, right, ((1,), (0,))) * solved
    else:
        product = dot(scatter, solved, ((1,), (0,))) * solved
    epoch_ref[...] = (jnp.sum(product, axis=0, keepdims=True) * (1.0 / npixels))[0, 0:epochs]

    if 6 * epochs <= 256:
        fitted = split_dot(system, data)
    else:
        fitted = dot(system, data, ((0,), (0,)))
    fitted = fitted[epochs : epochs + columns, :]
    for q in range(block):
        coefficients_ref[:, q, :] = fitted[:, q * width : (q + 1) * width]


HUB = 1


def ceil_to(value, unit):
    return -(-value // unit) * unit


def solution(mesh):
    n = mesh.shape["ep"]

    def shards(images, reference_image, kernels, kernel_index, tile_mask, systematics, onsets):
        local, rows, width = images.shape
        side = kernels.shape[1]
        tiles = width // LANES
        block = rows // n
        epochs = local * n
        columns = systematics.shape[1] + onsets.shape[0]
        pack = max(LANES // epochs, 1)
        share = epochs // pack
        part_lanes = max(LANES, epochs)
        vmem = pl.BlockSpec(memory_space=pltpu.VMEM)
        dma = pltpu.SemaphoreType.DMA
        f32 = jnp.float32
        flat_kernels = jnp.transpose(kernels, (1, 0, 2))
        flat_mask = jnp.transpose(tile_mask, (0, 2, 1))
        system_lanes = ceil_to(2 * epochs + columns, LANES)
        pieces = rows * tiles
        strips = block * tiles
        pixels, total, system = pl.pallas_call(
            functools.partial(exchange_kernel, n, HUB),
            out_shape=(
                jax.ShapeDtypeStruct((strips, n, local, LANES), f32),
                jax.ShapeDtypeStruct((epochs, part_lanes), f32),
                jax.ShapeDtypeStruct((epochs, system_lanes), f32),
            ),
            in_specs=[pl.BlockSpec(memory_space=pltpu.HBM)] * 7,
            out_specs=(vmem, vmem, vmem),
            scratch_shapes=[
                pltpu.VMEM(images.shape, f32),
                pltpu.VMEM(reference_image.shape, f32),
                pltpu.VMEM((ceil_to(side, 8), *flat_kernels.shape[1:]), f32),
                pltpu.SMEM(kernel_index.shape, jnp.int32),
                pltpu.VMEM(flat_mask.shape, jnp.int32),
                pltpu.VMEM(systematics.shape, f32),
                pltpu.SMEM(onsets.shape, jnp.int32),
                pltpu.VMEM((max(LANES, local * ceil_to(side + 8, 8)), LANES), f32),
                pltpu.VMEM((epochs, system_lanes), f32),
                pltpu.VMEM((rows * tiles * local, LANES), f32),
                pltpu.VMEM((pieces, n, local, LANES), f32),
                pltpu.VMEM((n, share, part_lanes), f32),
                pltpu.VMEM((share, part_lanes), f32),
                pltpu.SemaphoreType.DMA((7,)),
                pltpu.SemaphoreType.REGULAR,
                dma,
                dma,
                dma,
                dma,
                dma,
                dma,
                dma,
            ],
            compiler_params=pltpu.CompilerParams(
                collective_id=0, has_side_effects=True, vmem_limit_bytes=VMEM_GRANT
            ),
        )(
            *(
                pltpu.with_memory_space_constraint(value, pltpu.HBM)
                for value in (
                    images,
                    reference_image,
                    flat_kernels,
                    kernel_index,
                    flat_mask,
                    systematics,
                    onsets,
                )
            )
        )
        return pl.pallas_call(
            functools.partial(fit_kernel, float(rows * width)),
            out_shape=(
                jax.ShapeDtypeStruct((columns, block, width), f32),
                jax.ShapeDtypeStruct((epochs,), f32),
            ),
            in_specs=[vmem, vmem, vmem],
            out_specs=(vmem, vmem),
            compiler_params=pltpu.CompilerParams(vmem_limit_bytes=VMEM_GRANT),
        )(pixels, total, system)

    in_specs = (
        P(("field", "ep"), None, None),
        P("field", None),
        P(),
        P(("field", "ep")),
        P(("field", "ep"), None, None),
        P("field", None),
        P("field"),
    )
    out_specs = (P(None, ("field", "ep"), None), P("field"))
    return jax.shard_map(shards, mesh=mesh, in_specs=in_specs, out_specs=out_specs, check_vma=False)
```

```python
import functools

import jax
import jax.numpy as jnp
from jax import lax
from jax.experimental import pallas as pl
from jax.experimental.pallas import tpu as pltpu
from jax.sharding import PartitionSpec as P

cov_ridge = 0.5
fit_ridge = 1.0
LANES = 128
GROUP = 8
VMEM_GRANT = 24 * 2**20
HIGHEST = lax.Precision.HIGHEST


def dot(a, b, contract, precision=HIGHEST):
    return lax.dot_general(
        a, b, ((contract[0], contract[1]), ((), ())), precision=precision, preferred_element_type=jnp.float32
    )


def iota(shape, axis):
    return lax.broadcasted_iota(jnp.int32, shape, axis)


def cut(value, count):
    parts = []
    for _ in range(count - 1):
        parts.append(value.astype(jnp.bfloat16))
        value = value - parts[-1].astype(jnp.float32)
    return [*parts, value.astype(jnp.bfloat16)]


def plain_dot(a, b, contract):
    return lax.dot_general(
        a, b, ((contract[0], contract[1]), ((), ())), preferred_element_type=jnp.float32
    )


def turn(value, shift, stride):
    shift %= LANES
    if stride >= 0 and shift + 7 * stride <= LANES:
        return pltpu.roll(value, shift, axis=1, stride=stride, stride_axis=0)
    index = (iota(value.shape, 1) - shift - stride * iota(value.shape, 0)) & (LANES - 1)
    return jnp.take_along_axis(value, index, axis=1)


def spread(value, row):
    return jnp.broadcast_to(value[row : row + 1, :], value.shape)


def column(value, at):
    lanes = value.shape[1]
    tile = at // LANES * LANES
    value = value[:, tile : tile + LANES]
    value = jnp.take_along_axis(value, jnp.full((8, LANES), at - tile, jnp.int32), axis=1)
    return jnp.concatenate([value] * (lanes // LANES), axis=1)


def total_of(terms):
    while len(terms) > 1:
        terms = [p + q for p, q in zip(terms[0::2], terms[1::2])]
    return terms[0]


def eliminate(values, at):
    size = len(values)
    index = iota(values[0].shape, 0)
    spans = [[column(value, at + k) for value in values] for k in range(8 * size)]
    for first_row in range(0, 8 * size, 2):
        owner, row = divmod(first_row, 8)
        lefts, rights = spans[first_row], spans[first_row + 1]
        a, b = spread(lefts[owner], row), spread(rights[owner], row)
        c, d = spread(lefts[owner], row + 1), spread(rights[owner], row + 1)
        inverse = 1.0 / (a * d - b * c)
        upper, lower = index == row, index == row + 1
        pair = upper | lower
        weights = []
        for i in range(size):
            one, two = rights[i] * c - lefts[i] * d, lefts[i] * b - rights[i] * a
            if i == owner:
                one = jnp.where(upper, d, jnp.where(lower, -c, one))
                two = jnp.where(upper, -b, jnp.where(lower, a, two))
            weights.append((one * inverse, two * inverse))

        def step(values):
            first, second = spread(values[owner], row), spread(values[owner], row + 1)
            return [
                (jnp.where(pair, 0.0, value) if i == owner else value)
                + weights[i][0] * first
                + weights[i][1] * second
                for i, value in enumerate(values)
            ]

        spans = [step(span) if j > first_row + 1 else span for j, span in enumerate(spans)]
        values = step(values)
    return values


def invert_early(square, base, npixels, inverse_ref):
    count, lanes = square.shape
    epochs = base.shape[0]
    lane = iota((count, lanes), 1)
    matrix = (square + pltpu.roll(square, lanes - count, axis=1)) * (1.0 / npixels)
    matrix = matrix + pltpu.roll(base[0:count, :], epochs, axis=1)
    unit = jnp.where(lane - count == iota((count, lanes), 0), 1.0, 0.0)
    system = jnp.where(lane < count, matrix, unit)
    values = eliminate([system[i : i + 8, :] for i in range(0, count, 8)], 0)
    for i, value in enumerate(values):
        for k in range(count):
            inverse_ref[i * count + k] = column(value, count + k)


def solve(total, base, npixels, inverse_ref):
    epochs, lanes = base.shape
    lane = iota((epochs, lanes), 1)
    covariance = jnp.concatenate([total] * (lanes // total.shape[1]), axis=1) * (1.0 / npixels)
    ends = (lane < epochs) | (lane >= lanes - epochs)
    system = base + jnp.where(ends, covariance, 0.0)
    strips = [system[i : i + 8, :] for i in range(0, epochs, 8)]
    size = 2 if epochs % 16 == 0 else 1
    for start in range(0, epochs // 8, size):
        home = range(start, start + size)
        order = [i for i in range(epochs // 8) if i not in home]
        at = lanes - epochs + start * 8
        factors = [[column(strips[i], at + k) for k in range(8 * size)] for i in order]
        values = [strips[i] for i in home]
        if inverse_ref is not None and start == 0:
            count = 8 * size
            pivots = [spread(values[k // 8], k % 8) for k in range(count)]
            values = [
                total_of([inverse_ref[i * count + k] * pivots[k] for k in range(count)])
                for i in range(size)
            ]
        else:
            values = eliminate(values, at)
        pivots = [spread(values[k // 8], k % 8) for k in range(8 * size)]
        for i, factor in zip(order, factors):
            strips[i] = strips[i] - total_of([p * q for p, q in zip(factor, pivots)])
        for i, value in zip(home, values):
            strips[i] = value
    return jnp.concatenate(strips, axis=0)


def exchange_kernel(
    n,
    hub,
    images_hbm,
    reference_hbm,
    kernels_hbm,
    index_hbm,
    mask_hbm,
    systematics_hbm,
    onsets_hbm,
    pixels,
    total_ref,
    system_ref,
    images_ref,
    reference_ref,
    kernels_ref,
    index_ref,
    mask_ref,
    systematics_ref,
    onsets_ref,
    table,
    work,
    send,
    recv,
    spare,
    packed_ref,
    early_ref,
    inverse_ref,
    load_sem,
    ready_sem,
    row_sem,
    hub_sem,
    total_sem,
    early_sem,
    early_send_sem,
    hub_send_sem,
    row_send_sem,
    total_send_sem,
    mate_send_sem,
):
    local, rows, width = images_ref.shape
    side = kernels_hbm.shape[0]
    nk = kernels_hbm.shape[1]
    choices = kernels_ref.reshape(kernels_ref.shape[0] * nk, side)
    half = (side - 1) // 2
    tiles = width // LANES
    block = rows // n
    epochs = local * n
    nsys = systematics_ref.shape[1]
    ntr = onsets_ref.shape[0]
    columns = nsys + ntr
    pack = max(LANES // epochs, 1)
    me = lax.axis_index("ep")
    mate = hub - 1
    pieces = recv.shape[0]
    strips = block * tiles
    share = epochs // pack
    strip = iota((share, total_ref.shape[1]), 1) // epochs

    loads = [
        pltpu.make_async_copy(source, target, load_sem.at[i])
        for i, (source, target) in enumerate(
            (
                (index_hbm, index_ref),
                (kernels_hbm, kernels_ref.at[0:side]),
                (images_hbm, images_ref),
                (mask_hbm, mask_ref),
                (reference_hbm, reference_ref),
                (systematics_hbm, systematics_ref),
                (onsets_hbm, onsets_ref),
            )
        )
    ]
    for load in loads:
        load.start()

    def signal(semaphore, device):
        pl.semaphore_signal(
            semaphore, inc=1, device_id={"ep": device}, device_id_type=pl.DeviceIdType.MESH
        )

    barrier = pltpu.get_barrier_semaphore()

    @pl.when(me == hub)
    def _():
        for d in range(1, n):
            signal(barrier, lax.rem(me + d, n))

    @pl.when(me != hub)
    def _():
        signal(barrier, hub)

    table[...] = jnp.zeros_like(table)
    for load in loads:
        load.wait()

    steps = -(-side // GROUP)
    middle, offset = half // GROUP, half % GROUP
    depth = rows * GROUP
    lane = iota((8, LANES), 1)
    sublane = iota((8, LANES), 0)
    place = lane + sublane - offset
    banks = -(-side // 8)
    pages = -(-(GROUP * side + side) // LANES)
    turned = []
    for e in range(local):
        at = e * 8 * banks
        for g in range(banks):
            table[at + 8 * g : at + 8 * g + 8, 0:side] = choices[
                pl.ds(index_ref[e] + 8 * g * nk, 8, stride=nk), :
            ]
    for e in range(local):
        at = e * 8 * banks
        turned.append(
            [
                turn(table[at + 8 * g : at + 8 * g + 8, :], 8 * g * GROUP, GROUP)
                for g in range(banks)
            ]
        )
    windows = {}
    for m in range(steps):
        for page in range(pages):
            for g in range(banks):
                low = GROUP * (8 * g + m) - page * LANES
                if low + 8 * GROUP > 0 and low < LANES:
                    away = lane - GROUP * sublane - low
                    inside = (away >= 0) & (away < GROUP) & (sublane < side - 8 * g)
                    windows[m, page, g] = inside
    flats = {}
    for m in range(steps):
        for e in range(local):
            for page in range(pages):
                total = jnp.zeros((8, LANES), jnp.float32)
                for g in range(banks):
                    if (m, page, g) in windows:
                        total = total + jnp.where(windows[m, page, g], turned[e][g], 0.0)
                total = jnp.sum(total, axis=0, keepdims=True)
                flats[e, m, page] = jnp.broadcast_to(total, (8, LANES))
    bands = [[] for _ in range(local)]
    for m in range(steps):
        for h in range(rows // 8):
            for e in range(local):
                pieces_of = []
                for start in range(0, depth, LANES):
                    base = start + GROUP * (half + m - 8 * h)
                    spot = lane + base - GROUP * sublane
                    value = jnp.zeros((8, LANES), jnp.float32)
                    for page in range(pages):
                        if base + LANES <= page * LANES or base - 7 * GROUP >= (page + 1) * LANES:
                            continue
                        moved = turn(flats[e, m, page], -base, GROUP)
                        inside = (spot >= page * LANES) & (spot < (page + 1) * LANES)
                        value = jnp.where(inside, moved, value)
                    pieces_of.append(value)
                bands[e].append(jnp.concatenate(pieces_of, axis=1))
    good = {}
    for e in range(local):
        at = table.shape[0] - (e + 1) * 8
        table[at : at + tiles, 0:rows] = mask_ref[e].astype(jnp.float32)
        for t in range(tiles):
            row = jnp.broadcast_to(table[at + t : at + t + 1, :], (8, LANES))
            for r in range(0, rows, 8):
                good[e, t, r] = jnp.take_along_axis(row, sublane + r, axis=1)
    for e in range(local):
        spread_rows = []
        for r in range(rows):
            moved = [
                turn(
                    jnp.broadcast_to(
                        images_ref[e, r : r + 1, t * LANES : (t + 1) * LANES], (8, LANES)
                    ),
                    offset,
                    -1,
                )
                for t in range(tiles)
            ]
            moved.append(None)
            parts_of = []
            for t in range(tiles + 1):
                value = jnp.zeros((8, LANES), jnp.float32) if moved[t] is None else moved[t]
                before, after = moved[t - 1], moved[(t + 1) % (tiles + 1)]
                value = jnp.where(place < 0, 0.0 if before is None else before, value)
                value = jnp.where(place >= LANES, 0.0 if after is None else after, value)
                parts_of.append(value)
            spread_rows.append(jnp.concatenate(parts_of, axis=1))
        response = dot(
            jnp.concatenate(bands[e], axis=0),
            jnp.concatenate(spread_rows, axis=0),
            ((1,), (0,)),
            lax.Precision.HIGH,
        )
        span = width + LANES
        model = response[middle * rows : (middle + 1) * rows, 0:width]
        for m in range(steps):
            if m != middle:
                part = response[m * rows : (m + 1) * rows, :]
                model = model + pltpu.roll(part, (-GROUP * (m - middle)) % span, axis=1)[:, 0:width]
        difference = reference_ref[...] - model
        for t in range(tiles):
            for r in range(0, rows, 8):
                first = (r * tiles + t) * local + e
                piece = difference[r : r + 8, t * LANES : (t + 1) * LANES]
                send[pl.ds(first, 8, stride=tiles * local), :] = piece * good[e, t, r]

    sources = send.reshape(rows * tiles, local, LANES)
    def copy(source, target, semaphores, device):
        return pltpu.make_async_remote_copy(
            src_ref=source,
            dst_ref=target,
            send_sem=semaphores[0],
            recv_sem=semaphores[1],
            device_id={"ep": device},
            device_id_type=pl.DeviceIdType.MESH,
        )

    @pl.when(me != hub)
    def _():
        pl.semaphore_wait(barrier, 1)
        copy(sources, recv.at[:, me], (hub_send_sem, hub_sem.at[me // (n // 2)]), hub).start()

    @pl.when(me == hub)
    def _():
        pl.semaphore_wait(barrier, n - 1)
        for d in range(1, n):
            signal(ready_sem, lax.rem(me + d, n))
        recv[:, me] = sources[...]

    work[...] = jnp.zeros_like(work)
    epoch = iota((epochs, LANES), 0).astype(jnp.float32)
    template = iota((epochs, LANES), 1)
    onset = jnp.zeros((epochs, LANES), jnp.float32)
    for k in range(ntr):
        onset = jnp.where(template == k, onsets_ref[k].astype(jnp.float32), onset)
    delays = epoch - onset
    timescale = (template.astype(jnp.float32) + 1.0) * epochs / (2.0 * ntr)
    transient = jnp.where(delays >= 0.0, jnp.exp(-jnp.maximum(delays, 0.0) / timescale), 0.0)
    work[:, epochs : epochs + nsys] = systematics_ref[...]
    work[:, epochs + nsys : epochs + columns] = transient[:, 0:ntr]
    design = work[...]
    outer = dot(design, design, ((1,), (1,)))
    diagonal = iota((epochs, epochs), 0) == iota((epochs, epochs), 1)
    ridge = jnp.where(diagonal, cov_ridge, 0.0)
    lanes = work.shape[1]
    work[:, 0:epochs] = ridge
    work[:, lanes - epochs : lanes] = fit_ridge * outer + ridge

    def drain(ref, semaphore):
        pltpu.make_async_copy(ref, ref, semaphore).wait()

    @pl.when(me != hub)
    def _():
        pl.semaphore_wait(ready_sem, 1)

    for d in range(n - 2):
        device = 2 + lax.rem(me + d, n - 2)

        @pl.when(me != device)
        def _():
            rows_of = sources.at[pl.ds(device * strips, strips)]
            copy(rows_of, pixels.at[:, me], (row_send_sem, row_sem), device).start()

    @pl.when(me > hub)
    def _():
        pixels[:, me] = sources[pl.ds(me * strips, strips)]

    count = early_ref.shape[0]
    early = count * 2 == epochs
    gathered = recv.reshape(pieces, epochs, LANES)

    @pl.when(me == hub)
    def _():
        drain(recv.at[:, 0 : n // 2 - 1], hub_sem.at[0])
        if early:
            data = jnp.concatenate([gathered[i, 0:count, :] for i in range(pieces)], axis=1)
            both = jnp.concatenate(cut(data, 2), axis=0)
            square = plain_dot(both, both, ((1,), (1,)))
            early_ref[...] = jnp.zeros_like(early_ref)
            early_ref[:, 0 : 2 * count] = square[0:count] + square[count : 2 * count]
            for d in range(1, n):
                device = lax.rem(me + n - d, n)
                copy(early_ref, early_ref, (early_send_sem, early_sem), device).start()

    if early:

        @pl.when(me != hub)
        def _():
            drain(early_ref, early_sem)

        invert_early(early_ref[...], work[...], float(rows * width), inverse_ref)

    @pl.when(me == hub)
    def _():
        drain(recv.at[:, 0 : n // 2], hub_sem.at[1])
        copy(recv.at[mate * strips : hub * strips], pixels, (row_send_sem, row_sem), mate).start()
        step = min(pieces, 32)

        def gram(start):
            data = jnp.concatenate([gathered[start + i] for i in range(step)], axis=1)
            both = jnp.concatenate(cut(data, 2), axis=0)
            square = plain_dot(both, both, ((1,), (1,)))
            return square[0:epochs] + square[epochs : 2 * epochs]

        if step == pieces:
            square = gram(0)
        else:
            square = lax.fori_loop(
                0,
                pieces // step,
                lambda i, value: value + gram(i * step),
                jnp.zeros((epochs, 2 * epochs), jnp.float32),
            )
        if pack > 1:
            table[0:epochs, 2 * epochs :] = jnp.zeros((epochs, LANES - 2 * epochs), jnp.float32)
            table[0:epochs, 0 : 2 * epochs] = square
            wide = table[0:epochs, :]
            total = wide
            for j in range(1, pack):
                total = total + pltpu.roll(wide, j * epochs, axis=1)
            total_ref[...] = total
            packed = total[0:share, :]
            for j in range(1, pack):
                packed = jnp.where(strip == j, total[j * share : (j + 1) * share, :], packed)
            packed_ref[...] = packed
        else:
            total_ref[...] = square[:, 0:epochs] + square[:, epochs : 2 * epochs]
        for d in range(1, n):
            device = lax.rem(me + n - d, n)
            if d == 1 and pack > 1:
                copy(total_ref, total_ref, (mate_send_sem, total_sem), device).start()
            elif pack > 1:
                copy(packed_ref, packed_ref, (total_send_sem, total_sem), device).start()
            else:
                copy(total_ref, total_ref, (total_send_sem, total_sem), device).start()
        pixels[...] = recv[hub * strips : (hub + 1) * strips]

    @pl.when(me == mate)
    def _():
        drain(total_ref, total_sem)

    @pl.when(me > hub)
    def _():
        if pack > 1:
            drain(packed_ref, total_sem)
            packed = packed_ref[...]
            for j in range(pack):
                one = jnp.where(strip == j, packed, 0.0)
                total = one
                for k in range(1, pack):
                    total = total + pltpu.roll(one, k * epochs, axis=1)
                total_ref[j * share : (j + 1) * share, :] = total
        else:
            drain(total_ref, total_sem)

    system_ref[...] = solve(
        total_ref[...], work[...], float(rows * width), inverse_ref if early else None
    )

    @pl.when(me == mate)
    def _():
        drain(sources, hub_send_sem)
        drain(pixels, row_sem)
        drain(pixels.at[:, 0 : n - 2], row_send_sem)

    @pl.when(me > hub)
    def _():
        drain(sources, hub_send_sem)
        drain(pixels.at[:, 0 : n - 1], row_sem)
        drain(pixels.at[:, 0 : n - 3], row_send_sem)

    @pl.when(me == hub)
    def _():
        drain(recv.at[0 : 2 * strips, 0 : n - 1], row_send_sem)
        if early:
            drain(recv.at[0 : count // local, 0 : n - 1], early_send_sem)
        if pack > 1:
            drain(spare.at[0 : n - 2], total_send_sem)
            drain(total_ref, mate_send_sem)
        else:
            drain(spare.at[0 : n - 1], total_send_sem)


def split_dot(a, b):
    high, middle, low = cut(a, 3)
    left = jnp.concatenate([high, high, middle, high, middle, low], axis=0)
    high, middle, low = cut(b, 3)
    right = jnp.concatenate([high, middle, high, low, middle, high], axis=0)
    return plain_dot(left, right, ((0,), (0,)))


def fit_kernel(npixels, pixels_ref, total_ref, system_ref, coefficients_ref, epoch_ref):
    columns, block, width = coefficients_ref.shape
    strips, n, local, _ = pixels_ref.shape
    epochs = n * local
    rows_of = pixels_ref.reshape(strips, epochs, LANES)
    data = jnp.concatenate([rows_of[i] for i in range(strips)], axis=1)
    total = total_ref[...]
    system = system_ref[...]

    solved = system[:, 0:LANES] if epochs < LANES else system[:, 0:epochs]
    scatter = total[:, 0:epochs]
    if epochs * 4 == total.shape[1]:
        parts = [part.astype(jnp.float32) for part in cut(total, 3)]
        high, middle, low = parts
        block_of = iota(total.shape, 1) // epochs
        front = jnp.where(block_of == 2, middle, high)
        back = jnp.where(block_of == 0, middle, jnp.where(block_of == 1, low, 0.0))
        left = jnp.concatenate([front, back], axis=1).astype(jnp.bfloat16)
        high, middle, low = cut(solved, 3)
        right = jnp.concatenate([high, middle, high, low, middle, high, high, high], axis=0)
        product = plain_dot(left, right, ((1,), (0,))) * solved
    else:
        product = dot(scatter, solved, ((1,), (0,))) * solved
    epoch_ref[...] = (jnp.sum(product, axis=0, keepdims=True) * (1.0 / npixels))[0, 0:epochs]

    if 6 * epochs <= 256:
        fitted = split_dot(system, data)
    else:
        fitted = dot(system, data, ((0,), (0,)))
    fitted = fitted[epochs : epochs + columns, :]
    for q in range(block):
        coefficients_ref[:, q, :] = fitted[:, q * width : (q + 1) * width]


HUB = 1
EARLY = 16


def ceil_to(value, unit):
    return -(-value // unit) * unit


def solution(mesh):
    n = mesh.shape["ep"]

    def shards(images, reference_image, kernels, kernel_index, tile_mask, systematics, onsets):
        local, rows, width = images.shape
        side = kernels.shape[1]
        tiles = width // LANES
        block = rows // n
        epochs = local * n
        columns = systematics.shape[1] + onsets.shape[0]
        pack = max(LANES // epochs, 1)
        share = epochs // pack
        part_lanes = max(LANES, epochs)
        vmem = pl.BlockSpec(memory_space=pltpu.VMEM)
        dma = pltpu.SemaphoreType.DMA
        f32 = jnp.float32
        flat_kernels = jnp.transpose(kernels, (1, 0, 2))
        flat_mask = jnp.transpose(tile_mask, (0, 2, 1))
        system_lanes = ceil_to(2 * epochs + columns, LANES)
        pieces = rows * tiles
        strips = block * tiles
        pixels, total, system = pl.pallas_call(
            functools.partial(exchange_kernel, n, HUB),
            out_shape=(
                jax.ShapeDtypeStruct((strips, n, local, LANES), f32),
                jax.ShapeDtypeStruct((epochs, part_lanes), f32),
                jax.ShapeDtypeStruct((epochs, system_lanes), f32),
            ),
            in_specs=[pl.BlockSpec(memory_space=pltpu.HBM)] * 7,
            out_specs=(vmem, vmem, vmem),
            scratch_shapes=[
                pltpu.VMEM(images.shape, f32),
                pltpu.VMEM(reference_image.shape, f32),
                pltpu.VMEM((ceil_to(side, 8), *flat_kernels.shape[1:]), f32),
                pltpu.SMEM(kernel_index.shape, jnp.int32),
                pltpu.VMEM(flat_mask.shape, jnp.int32),
                pltpu.VMEM(systematics.shape, f32),
                pltpu.SMEM(onsets.shape, jnp.int32),
                pltpu.VMEM((max(LANES, local * ceil_to(side + 8, 8)), LANES), f32),
                pltpu.VMEM((epochs, system_lanes), f32),
                pltpu.VMEM((rows * tiles * local, LANES), f32),
                pltpu.VMEM((pieces, n, local, LANES), f32),
                pltpu.VMEM((n, share, part_lanes), f32),
                pltpu.VMEM((share, part_lanes), f32),
                pltpu.VMEM((EARLY, LANES), f32),
                pltpu.VMEM((2 * EARLY, 8, LANES), f32),
                pltpu.SemaphoreType.DMA((7,)),
                pltpu.SemaphoreType.REGULAR,
                dma,
                pltpu.SemaphoreType.DMA((2,)),
                dma,
                dma,
                dma,
                dma,
                dma,
                dma,
                dma,
            ],
            compiler_params=pltpu.CompilerParams(
                collective_id=0, has_side_effects=True, vmem_limit_bytes=VMEM_GRANT
            ),
        )(
            *(
                pltpu.with_memory_space_constraint(value, pltpu.HBM)
                for value in (
                    images,
                    reference_image,
                    flat_kernels,
                    kernel_index,
                    flat_mask,
                    systematics,
                    onsets,
                )
            )
        )
        return pl.pallas_call(
            functools.partial(fit_kernel, float(rows * width)),
            out_shape=(
                jax.ShapeDtypeStruct((columns, block, width), f32),
                jax.ShapeDtypeStruct((epochs,), f32),
            ),
            in_specs=[vmem, vmem, vmem],
            out_specs=(vmem, vmem),
            compiler_params=pltpu.CompilerParams(vmem_limit_bytes=VMEM_GRANT),
        )(pixels, total, system)

    in_specs = (
        P(("field", "ep"), None, None),
        P("field", None),
        P(),
        P(("field", "ep")),
        P(("field", "ep"), None, None),
        P("field", None),
        P("field"),
    )
    out_specs = (P(None, ("field", "ep"), None), P("field"))
    return jax.shard_map(shards, mesh=mesh, in_specs=in_specs, out_specs=out_specs, check_vma=False)
```

```python
import functools

import jax
import jax.numpy as jnp
from jax import lax
from jax.experimental import pallas as pl
from jax.experimental.pallas import tpu as pltpu
from jax.sharding import PartitionSpec as P

cov_ridge = 0.5
fit_ridge = 1.0
LANES = 128
GROUP = 8
VMEM_GRANT = 24 * 2**20
HIGHEST = lax.Precision.HIGHEST


def dot(a, b, contract, precision=HIGHEST):
    return lax.dot_general(
        a, b, ((contract[0], contract[1]), ((), ())), precision=precision, preferred_element_type=jnp.float32
    )


def iota(shape, axis):
    return lax.broadcasted_iota(jnp.int32, shape, axis)


def cut(value, count):
    parts = []
    for _ in range(count - 1):
        parts.append(value.astype(jnp.bfloat16))
        value = value - parts[-1].astype(jnp.float32)
    return [*parts, value.astype(jnp.bfloat16)]


def plain_dot(a, b, contract):
    return lax.dot_general(
        a, b, ((contract[0], contract[1]), ((), ())), preferred_element_type=jnp.float32
    )


def turn(value, shift, stride):
    shift %= LANES
    if stride >= 0 and shift + 7 * stride <= LANES:
        return pltpu.roll(value, shift, axis=1, stride=stride, stride_axis=0)
    index = (iota(value.shape, 1) - shift - stride * iota(value.shape, 0)) & (LANES - 1)
    return jnp.take_along_axis(value, index, axis=1)


def spread(value, row):
    return jnp.broadcast_to(value[row : row + 1, :], value.shape)


def column(value, at):
    lanes = value.shape[1]
    tile = at // LANES * LANES
    value = value[:, tile : tile + LANES]
    value = jnp.take_along_axis(value, jnp.full((8, LANES), at - tile, jnp.int32), axis=1)
    return jnp.concatenate([value] * (lanes // LANES), axis=1)


def total_of(terms):
    while len(terms) > 1:
        terms = [p + q for p, q in zip(terms[0::2], terms[1::2])]
    return terms[0]


def eliminate(values, at):
    size = len(values)
    index = iota(values[0].shape, 0)
    spans = [[column(value, at + k) for value in values] for k in range(8 * size)]
    for first_row in range(0, 8 * size, 2):
        owner, row = divmod(first_row, 8)
        lefts, rights = spans[first_row], spans[first_row + 1]
        a, b = spread(lefts[owner], row), spread(rights[owner], row)
        c, d = spread(lefts[owner], row + 1), spread(rights[owner], row + 1)
        inverse = 1.0 / (a * d - b * c)
        upper, lower = index == row, index == row + 1
        pair = upper | lower
        weights = []
        for i in range(size):
            one, two = rights[i] * c - lefts[i] * d, lefts[i] * b - rights[i] * a
            if i == owner:
                one = jnp.where(upper, d, jnp.where(lower, -c, one))
                two = jnp.where(upper, -b, jnp.where(lower, a, two))
            weights.append((one * inverse, two * inverse))

        def step(values):
            first, second = spread(values[owner], row), spread(values[owner], row + 1)
            return [
                (jnp.where(pair, 0.0, value) if i == owner else value)
                + weights[i][0] * first
                + weights[i][1] * second
                for i, value in enumerate(values)
            ]

        spans = [step(span) if j > first_row + 1 else span for j, span in enumerate(spans)]
        values = step(values)
    return values


def invert_early(square, base, npixels, inverse_ref):
    count, lanes = square.shape
    epochs = base.shape[0]
    lane = iota((count, lanes), 1)
    matrix = (square + pltpu.roll(square, lanes - count, axis=1)) * (1.0 / npixels)
    matrix = matrix + pltpu.roll(base[0:count, :], epochs, axis=1)
    unit = jnp.where(lane - count == iota((count, lanes), 0), 1.0, 0.0)
    system = jnp.where(lane < count, matrix, unit)
    values = eliminate([system[i : i + 8, :] for i in range(0, count, 8)], 0)
    for i, value in enumerate(values):
        for k in range(count):
            inverse_ref[i * count + k] = column(value, count + k)


def solve(total, base, npixels, inverse_ref):
    epochs, lanes = base.shape
    lane = iota((epochs, lanes), 1)
    covariance = jnp.concatenate([total] * (lanes // total.shape[1]), axis=1) * (1.0 / npixels)
    ends = (lane < epochs) | (lane >= lanes - epochs)
    system = base + jnp.where(ends, covariance, 0.0)
    strips = [system[i : i + 8, :] for i in range(0, epochs, 8)]
    size = 2 if epochs % 16 == 0 else 1
    for start in range(0, epochs // 8, size):
        home = range(start, start + size)
        order = [i for i in range(epochs // 8) if i not in home]
        at = lanes - epochs + start * 8
        factors = [[column(strips[i], at + k) for k in range(8 * size)] for i in order]
        values = [strips[i] for i in home]
        if inverse_ref is not None and start == 0:
            count = 8 * size
            pivots = [spread(values[k // 8], k % 8) for k in range(count)]
            values = [
                total_of([inverse_ref[i * count + k] * pivots[k] for k in range(count)])
                for i in range(size)
            ]
        else:
            values = eliminate(values, at)
        pivots = [spread(values[k // 8], k % 8) for k in range(8 * size)]
        for i, factor in zip(order, factors):
            strips[i] = strips[i] - total_of([p * q for p, q in zip(factor, pivots)])
        for i, value in zip(home, values):
            strips[i] = value
    return jnp.concatenate(strips, axis=0)


def exchange_kernel(
    n,
    hub,
    images_hbm,
    reference_hbm,
    kernels_hbm,
    index_hbm,
    mask_hbm,
    systematics_hbm,
    onsets_hbm,
    pixels,
    total_ref,
    system_ref,
    images_ref,
    reference_ref,
    kernels_ref,
    index_ref,
    mask_ref,
    systematics_ref,
    onsets_ref,
    table,
    work,
    send,
    recv,
    spare,
    packed_ref,
    early_ref,
    inverse_ref,
    load_sem,
    ready_sem,
    row_sem,
    hub_sem,
    total_sem,
    early_sem,
):
    local, rows, width = images_ref.shape
    side = kernels_hbm.shape[0]
    nk = kernels_hbm.shape[1]
    choices = kernels_ref.reshape(kernels_ref.shape[0] * nk, side)
    half = (side - 1) // 2
    tiles = width // LANES
    block = rows // n
    epochs = local * n
    nsys = systematics_ref.shape[1]
    ntr = onsets_ref.shape[0]
    columns = nsys + ntr
    pack = max(LANES // epochs, 1)
    me = lax.axis_index("ep")
    hub_send_sem, row_send_sem, total_send_sem, mate_send_sem, early_send_sem = (
        load_sem.at[i] for i in range(5)
    )
    mate = hub - 1
    pieces = recv.shape[0]
    strips = block * tiles
    share = epochs // pack
    strip = iota((share, total_ref.shape[1]), 1) // epochs

    loads = [
        pltpu.make_async_copy(source, target, load_sem.at[i])
        for i, (source, target) in enumerate(
            (
                (index_hbm, index_ref),
                (kernels_hbm, kernels_ref.at[0:side]),
                (images_hbm, images_ref),
                (mask_hbm, mask_ref),
                (reference_hbm, reference_ref),
                (systematics_hbm, systematics_ref),
                (onsets_hbm, onsets_ref),
            )
        )
    ]
    for load in loads:
        load.start()

    def signal(semaphore, device):
        pl.semaphore_signal(
            semaphore, inc=1, device_id={"ep": device}, device_id_type=pl.DeviceIdType.MESH
        )

    barrier = pltpu.get_barrier_semaphore()

    @pl.when(me == hub)
    def _():
        for d in range(1, n):
            signal(barrier, lax.rem(me + d, n))

    @pl.when(me != hub)
    def _():
        signal(barrier, hub)

    table[...] = jnp.zeros_like(table)
    for load in loads:
        load.wait()

    steps = -(-side // GROUP)
    middle, offset = half // GROUP, half % GROUP
    depth = rows * GROUP
    lane = iota((8, LANES), 1)
    sublane = iota((8, LANES), 0)
    place = lane + sublane - offset
    banks = -(-side // 8)
    pages = -(-(GROUP * side + side) // LANES)
    turned = []
    for e in range(local):
        at = e * 8 * banks
        for g in range(banks):
            table[at + 8 * g : at + 8 * g + 8, 0:side] = choices[
                pl.ds(index_ref[e] + 8 * g * nk, 8, stride=nk), :
            ]
    for e in range(local):
        at = e * 8 * banks
        turned.append(
            [
                turn(table[at + 8 * g : at + 8 * g + 8, :], 8 * g * GROUP, GROUP)
                for g in range(banks)
            ]
        )
    windows = {}
    for m in range(steps):
        for page in range(pages):
            for g in range(banks):
                low = GROUP * (8 * g + m) - page * LANES
                if low + 8 * GROUP > 0 and low < LANES:
                    away = lane - GROUP * sublane - low
                    inside = (away >= 0) & (away < GROUP) & (sublane < side - 8 * g)
                    windows[m, page, g] = inside
    flats = {}
    for m in range(steps):
        for e in range(local):
            for page in range(pages):
                total = jnp.zeros((8, LANES), jnp.float32)
                for g in range(banks):
                    if (m, page, g) in windows:
                        total = total + jnp.where(windows[m, page, g], turned[e][g], 0.0)
                total = jnp.sum(total, axis=0, keepdims=True)
                flats[e, m, page] = jnp.broadcast_to(total, (8, LANES))
    bands = [[] for _ in range(local)]
    for m in range(steps):
        for h in range(rows // 8):
            for e in range(local):
                pieces_of = []
                for start in range(0, depth, LANES):
                    base = start + GROUP * (half + m - 8 * h)
                    spot = lane + base - GROUP * sublane
                    value = jnp.zeros((8, LANES), jnp.float32)
                    for page in range(pages):
                        if base + LANES <= page * LANES or base - 7 * GROUP >= (page + 1) * LANES:
                            continue
                        moved = turn(flats[e, m, page], -base, GROUP)
                        inside = (spot >= page * LANES) & (spot < (page + 1) * LANES)
                        value = jnp.where(inside, moved, value)
                    pieces_of.append(value)
                bands[e].append(jnp.concatenate(pieces_of, axis=1))
    good = {}
    for e in range(local):
        at = table.shape[0] - (e + 1) * 8
        table[at : at + tiles, 0:rows] = mask_ref[e].astype(jnp.float32)
        for t in range(tiles):
            row = jnp.broadcast_to(table[at + t : at + t + 1, :], (8, LANES))
            for r in range(0, rows, 8):
                good[e, t, r] = jnp.take_along_axis(row, sublane + r, axis=1)
    for e in range(local):
        spread_rows = []
        for r in range(rows):
            moved = [
                turn(
                    jnp.broadcast_to(
                        images_ref[e, r : r + 1, t * LANES : (t + 1) * LANES], (8, LANES)
                    ),
                    offset,
                    -1,
                )
                for t in range(tiles)
            ]
            moved.append(None)
            parts_of = []
            for t in range(tiles + 1):
                value = jnp.zeros((8, LANES), jnp.float32) if moved[t] is None else moved[t]
                before, after = moved[t - 1], moved[(t + 1) % (tiles + 1)]
                value = jnp.where(place < 0, 0.0 if before is None else before, value)
                value = jnp.where(place >= LANES, 0.0 if after is None else after, value)
                parts_of.append(value)
            spread_rows.append(jnp.concatenate(parts_of, axis=1))
        response = dot(
            jnp.concatenate(bands[e], axis=0),
            jnp.concatenate(spread_rows, axis=0),
            ((1,), (0,)),
            lax.Precision.HIGH,
        )
        span = width + LANES
        model = response[middle * rows : (middle + 1) * rows, 0:width]
        for m in range(steps):
            if m != middle:
                part = response[m * rows : (m + 1) * rows, :]
                model = model + pltpu.roll(part, (-GROUP * (m - middle)) % span, axis=1)[:, 0:width]
        difference = reference_ref[...] - model
        for t in range(tiles):
            for r in range(0, rows, 8):
                first = (r * tiles + t) * local + e
                piece = difference[r : r + 8, t * LANES : (t + 1) * LANES]
                send[pl.ds(first, 8, stride=tiles * local), :] = piece * good[e, t, r]

    sources = send.reshape(rows * tiles, local, LANES)
    def copy(source, target, semaphores, device):
        return pltpu.make_async_remote_copy(
            src_ref=source,
            dst_ref=target,
            send_sem=semaphores[0],
            recv_sem=semaphores[1],
            device_id={"ep": device},
            device_id_type=pl.DeviceIdType.MESH,
        )

    @pl.when(me != hub)
    def _():
        pl.semaphore_wait(barrier, 1)
        copy(sources, recv.at[:, me], (hub_send_sem, hub_sem.at[me // (n // 2)]), hub).start()

    @pl.when(me == hub)
    def _():
        pl.semaphore_wait(barrier, n - 1)
        for d in range(1, n):
            signal(ready_sem, lax.rem(me + d, n))
        recv[:, me] = sources[...]

    work[...] = jnp.zeros_like(work)
    epoch = iota((epochs, LANES), 0).astype(jnp.float32)
    template = iota((epochs, LANES), 1)
    onset = jnp.zeros((epochs, LANES), jnp.float32)
    for k in range(ntr):
        onset = jnp.where(template == k, onsets_ref[k].astype(jnp.float32), onset)
    delays = epoch - onset
    timescale = (template.astype(jnp.float32) + 1.0) * epochs / (2.0 * ntr)
    transient = jnp.where(delays >= 0.0, jnp.exp(-jnp.maximum(delays, 0.0) / timescale), 0.0)
    work[:, epochs : epochs + nsys] = systematics_ref[...]
    work[:, epochs + nsys : epochs + columns] = transient[:, 0:ntr]
    design = work[...]
    outer = dot(design, design, ((1,), (1,)))
    diagonal = iota((epochs, epochs), 0) == iota((epochs, epochs), 1)
    ridge = jnp.where(diagonal, cov_ridge, 0.0)
    lanes = work.shape[1]
    work[:, 0:epochs] = ridge
    work[:, lanes - epochs : lanes] = fit_ridge * outer + ridge

    def drain(ref, semaphore):
        pltpu.make_async_copy(ref, ref, semaphore).wait()

    @pl.when(me != hub)
    def _():
        pl.semaphore_wait(ready_sem, 1)

    for d in range(n - 2):
        device = 2 + lax.rem(me + d, n - 2)

        @pl.when(me != device)
        def _():
            rows_of = sources.at[pl.ds(device * strips, strips)]
            copy(rows_of, pixels.at[:, me], (row_send_sem, row_sem), device).start()

    @pl.when(me > hub)
    def _():
        pixels[:, me] = sources[pl.ds(me * strips, strips)]

    count = early_ref.shape[0]
    early = count * 2 == epochs
    gathered = recv.reshape(pieces, epochs, LANES)

    @pl.when(me == hub)
    def _():
        drain(recv.at[:, 0 : n // 2 - 1], hub_sem.at[0])
        if early:
            data = jnp.concatenate([gathered[i, 0:count, :] for i in range(pieces)], axis=1)
            both = jnp.concatenate(cut(data, 2), axis=0)
            square = plain_dot(both, both, ((1,), (1,)))
            early_ref[...] = jnp.zeros_like(early_ref)
            early_ref[:, 0 : 2 * count] = square[0:count] + square[count : 2 * count]
            for d in range(1, n):
                device = lax.rem(me + n - d, n)
                copy(early_ref, early_ref, (early_send_sem, early_sem), device).start()

    if early:

        @pl.when(me != hub)
        def _():
            drain(early_ref, early_sem)

        invert_early(early_ref[...], work[...], float(rows * width), inverse_ref)

    @pl.when(me == hub)
    def _():
        drain(recv.at[:, 0 : n // 2], hub_sem.at[1])
        copy(recv.at[mate * strips : hub * strips], pixels, (row_send_sem, row_sem), mate).start()
        step = min(pieces, 32)

        def gram(start):
            data = jnp.concatenate([gathered[start + i] for i in range(step)], axis=1)
            both = jnp.concatenate(cut(data, 2), axis=0)
            square = plain_dot(both, both, ((1,), (1,)))
            return square[0:epochs] + square[epochs : 2 * epochs]

        if step == pieces:
            square = gram(0)
        else:
            square = lax.fori_loop(
                0,
                pieces // step,
                lambda i, value: value + gram(i * step),
                jnp.zeros((epochs, 2 * epochs), jnp.float32),
            )
        if pack > 1:
            table[0:epochs, 2 * epochs :] = jnp.zeros((epochs, LANES - 2 * epochs), jnp.float32)
            table[0:epochs, 0 : 2 * epochs] = square
            wide = table[0:epochs, :]
            total = wide
            for j in range(1, pack):
                total = total + pltpu.roll(wide, j * epochs, axis=1)
            total_ref[...] = total
            packed = total[0:share, :]
            for j in range(1, pack):
                packed = jnp.where(strip == j, total[j * share : (j + 1) * share, :], packed)
            packed_ref[...] = packed
        else:
            total_ref[...] = square[:, 0:epochs] + square[:, epochs : 2 * epochs]
        for d in range(1, n):
            device = lax.rem(me + n - d, n)
            if d == 1 and pack > 1:
                copy(total_ref, total_ref, (mate_send_sem, total_sem), device).start()
            elif pack > 1:
                copy(packed_ref, packed_ref, (total_send_sem, total_sem), device).start()
            else:
                copy(total_ref, total_ref, (total_send_sem, total_sem), device).start()
        pixels[...] = recv[hub * strips : (hub + 1) * strips]

    @pl.when(me == mate)
    def _():
        drain(total_ref, total_sem)

    @pl.when(me > hub)
    def _():
        if pack > 1:
            drain(packed_ref, total_sem)
            packed = packed_ref[...]
            for j in range(pack):
                one = jnp.where(strip == j, packed, 0.0)
                total = one
                for k in range(1, pack):
                    total = total + pltpu.roll(one, k * epochs, axis=1)
                total_ref[j * share : (j + 1) * share, :] = total
        else:
            drain(total_ref, total_sem)

    system_ref[...] = solve(
        total_ref[...], work[...], float(rows * width), inverse_ref if early else None
    )

    @pl.when(me == mate)
    def _():
        drain(sources, hub_send_sem)
        drain(pixels, row_sem)
        drain(pixels.at[:, 0 : n - 2], row_send_sem)

    @pl.when(me > hub)
    def _():
        drain(sources, hub_send_sem)
        drain(pixels.at[:, 0 : n - 1], row_sem)
        drain(pixels.at[:, 0 : n - 3], row_send_sem)

    @pl.when(me == hub)
    def _():
        drain(recv.at[0 : 2 * strips, 0 : n - 1], row_send_sem)
        if early:
            drain(recv.at[0 : count // local, 0 : n - 1], early_send_sem)
        if pack > 1:
            drain(spare.at[0 : n - 2], total_send_sem)
            drain(total_ref, mate_send_sem)
        else:
            drain(spare.at[0 : n - 1], total_send_sem)


def split_dot(a, b):
    high, middle, low = cut(a, 3)
    left = jnp.concatenate([high, high, middle, high, middle, low], axis=0)
    high, middle, low = cut(b, 3)
    right = jnp.concatenate([high, middle, high, low, middle, high], axis=0)
    return plain_dot(left, right, ((0,), (0,)))


def fit_kernel(npixels, pixels_ref, total_ref, system_ref, coefficients_ref, epoch_ref):
    columns, block, width = coefficients_ref.shape
    strips, n, local, _ = pixels_ref.shape
    epochs = n * local
    rows_of = pixels_ref.reshape(strips, epochs, LANES)
    data = jnp.concatenate([rows_of[i] for i in range(strips)], axis=1)
    total = total_ref[...]
    system = system_ref[...]

    solved = system[:, 0:LANES] if epochs < LANES else system[:, 0:epochs]
    scatter = total[:, 0:epochs]
    if epochs * 4 == total.shape[1]:
        parts = [part.astype(jnp.float32) for part in cut(total, 3)]
        high, middle, low = parts
        block_of = iota(total.shape, 1) // epochs
        front = jnp.where(block_of == 2, middle, high)
        back = jnp.where(block_of == 0, middle, jnp.where(block_of == 1, low, 0.0))
        left = jnp.concatenate([front, back], axis=1).astype(jnp.bfloat16)
        high, middle, low = cut(solved, 3)
        right = jnp.concatenate([high, middle, high, low, middle, high, high, high], axis=0)
        product = plain_dot(left, right, ((1,), (0,))) * solved
    else:
        product = dot(scatter, solved, ((1,), (0,))) * solved
    epoch_ref[...] = (jnp.sum(product, axis=0, keepdims=True) * (1.0 / npixels))[0, 0:epochs]

    if 6 * epochs <= 256:
        fitted = split_dot(system, data)
    else:
        fitted = dot(system, data, ((0,), (0,)))
    fitted = fitted[epochs : epochs + columns, :]
    for q in range(block):
        coefficients_ref[:, q, :] = fitted[:, q * width : (q + 1) * width]


HUB = 1
EARLY = 16


def ceil_to(value, unit):
    return -(-value // unit) * unit


def solution(mesh):
    n = mesh.shape["ep"]

    def shards(images, reference_image, kernels, kernel_index, tile_mask, systematics, onsets):
        local, rows, width = images.shape
        side = kernels.shape[1]
        tiles = width // LANES
        block = rows // n
        epochs = local * n
        columns = systematics.shape[1] + onsets.shape[0]
        pack = max(LANES // epochs, 1)
        share = epochs // pack
        part_lanes = max(LANES, epochs)
        vmem = pl.BlockSpec(memory_space=pltpu.VMEM)
        dma = pltpu.SemaphoreType.DMA
        f32 = jnp.float32
        flat_kernels = jnp.transpose(kernels, (1, 0, 2))
        flat_mask = jnp.transpose(tile_mask, (0, 2, 1))
        system_lanes = ceil_to(2 * epochs + columns, LANES)
        pieces = rows * tiles
        strips = block * tiles
        pixels, total, system = pl.pallas_call(
            functools.partial(exchange_kernel, n, HUB),
            out_shape=(
                jax.ShapeDtypeStruct((strips, n, local, LANES), f32),
                jax.ShapeDtypeStruct((epochs, part_lanes), f32),
                jax.ShapeDtypeStruct((epochs, system_lanes), f32),
            ),
            in_specs=[pl.BlockSpec(memory_space=pltpu.HBM)] * 7,
            out_specs=(vmem, vmem, vmem),
            scratch_shapes=[
                pltpu.VMEM(images.shape, f32),
                pltpu.VMEM(reference_image.shape, f32),
                pltpu.VMEM((ceil_to(side, 8), *flat_kernels.shape[1:]), f32),
                pltpu.SMEM(kernel_index.shape, jnp.int32),
                pltpu.VMEM(flat_mask.shape, jnp.int32),
                pltpu.VMEM(systematics.shape, f32),
                pltpu.SMEM(onsets.shape, jnp.int32),
                pltpu.VMEM((max(LANES, local * ceil_to(side + 8, 8)), LANES), f32),
                pltpu.VMEM((epochs, system_lanes), f32),
                pltpu.VMEM((rows * tiles * local, LANES), f32),
                pltpu.VMEM((pieces, n, local, LANES), f32),
                pltpu.VMEM((n, share, part_lanes), f32),
                pltpu.VMEM((share, part_lanes), f32),
                pltpu.VMEM((EARLY, LANES), f32),
                pltpu.VMEM((2 * EARLY, 8, LANES), f32),
                pltpu.SemaphoreType.DMA((7,)),
                pltpu.SemaphoreType.REGULAR,
                dma,
                pltpu.SemaphoreType.DMA((2,)),
                dma,
                dma,
            ],
            compiler_params=pltpu.CompilerParams(
                collective_id=0, has_side_effects=True, vmem_limit_bytes=VMEM_GRANT
            ),
        )(
            *(
                pltpu.with_memory_space_constraint(value, pltpu.HBM)
                for value in (
                    images,
                    reference_image,
                    flat_kernels,
                    kernel_index,
                    flat_mask,
                    systematics,
                    onsets,
                )
            )
        )
        return pl.pallas_call(
            functools.partial(fit_kernel, float(rows * width)),
            out_shape=(
                jax.ShapeDtypeStruct((columns, block, width), f32),
                jax.ShapeDtypeStruct((epochs,), f32),
            ),
            in_specs=[vmem, vmem, vmem],
            out_specs=(vmem, vmem),
            compiler_params=pltpu.CompilerParams(vmem_limit_bytes=VMEM_GRANT),
        )(pixels, total, system)

    in_specs = (
        P(("field", "ep"), None, None),
        P("field", None),
        P(),
        P(("field", "ep")),
        P(("field", "ep"), None, None),
        P("field", None),
        P("field"),
    )
    out_specs = (P(None, ("field", "ep"), None), P("field"))
    return jax.shard_map(shards, mesh=mesh, in_specs=in_specs, out_specs=out_specs, check_vma=False)
```

```python
import functools

import jax
import jax.numpy as jnp
from jax import lax
from jax.experimental import pallas as pl
from jax.experimental.pallas import tpu as pltpu
from jax.sharding import PartitionSpec as P

cov_ridge = 0.5
fit_ridge = 1.0
LANES = 128
GROUP = 8
VMEM_GRANT = 24 * 2**20
HIGHEST = lax.Precision.HIGHEST


def dot(a, b, contract, precision=HIGHEST):
    return lax.dot_general(
        a, b, ((contract[0], contract[1]), ((), ())), precision=precision, preferred_element_type=jnp.float32
    )


def iota(shape, axis):
    return lax.broadcasted_iota(jnp.int32, shape, axis)


def cut(value, count):
    parts = []
    for _ in range(count - 1):
        parts.append(value.astype(jnp.bfloat16))
        value = value - parts[-1].astype(jnp.float32)
    return [*parts, value.astype(jnp.bfloat16)]


def plain_dot(a, b, contract):
    return lax.dot_general(
        a, b, ((contract[0], contract[1]), ((), ())), preferred_element_type=jnp.float32
    )


def turn(value, shift, stride):
    shift %= LANES
    if stride >= 0 and shift + 7 * stride <= LANES:
        return pltpu.roll(value, shift, axis=1, stride=stride, stride_axis=0)
    index = (iota(value.shape, 1) - shift - stride * iota(value.shape, 0)) & (LANES - 1)
    return jnp.take_along_axis(value, index, axis=1)


def spread(value, row):
    return jnp.broadcast_to(value[row : row + 1, :], value.shape)


def column(value, at):
    lanes = value.shape[1]
    tile = at // LANES * LANES
    value = value[:, tile : tile + LANES]
    value = jnp.take_along_axis(value, jnp.full((8, LANES), at - tile, jnp.int32), axis=1)
    return jnp.concatenate([value] * (lanes // LANES), axis=1)


def total_of(terms):
    while len(terms) > 1:
        terms = [p + q for p, q in zip(terms[0::2], terms[1::2])]
    return terms[0]


def eliminate(values, at):
    size = len(values)
    index = iota(values[0].shape, 0)
    spans = [[column(value, at + k) for value in values] for k in range(8 * size)]
    for first_row in range(0, 8 * size, 2):
        owner, row = divmod(first_row, 8)
        lefts, rights = spans[first_row], spans[first_row + 1]
        a, b = spread(lefts[owner], row), spread(rights[owner], row)
        c, d = spread(lefts[owner], row + 1), spread(rights[owner], row + 1)
        inverse = 1.0 / (a * d - b * c)
        upper, lower = index == row, index == row + 1
        pair = upper | lower
        weights = []
        for i in range(size):
            one, two = rights[i] * c - lefts[i] * d, lefts[i] * b - rights[i] * a
            if i == owner:
                one = jnp.where(upper, d, jnp.where(lower, -c, one))
                two = jnp.where(upper, -b, jnp.where(lower, a, two))
            weights.append((one * inverse, two * inverse))

        def step(values):
            first, second = spread(values[owner], row), spread(values[owner], row + 1)
            return [
                (jnp.where(pair, 0.0, value) if i == owner else value)
                + weights[i][0] * first
                + weights[i][1] * second
                for i, value in enumerate(values)
            ]

        spans = [step(span) if j > first_row + 1 else span for j, span in enumerate(spans)]
        values = step(values)
    return values


def invert_early(square, base, npixels, inverse_ref):
    count, lanes = square.shape
    epochs = base.shape[0]
    lane = iota((count, lanes), 1)
    matrix = (square + pltpu.roll(square, lanes - count, axis=1)) * (1.0 / npixels)
    matrix = matrix + pltpu.roll(base[0:count, :], epochs, axis=1)
    unit = jnp.where(lane - count == iota((count, lanes), 0), 1.0, 0.0)
    system = jnp.where(lane < count, matrix, unit)
    values = eliminate([system[i : i + 8, :] for i in range(0, count, 8)], 0)
    for i, value in enumerate(values):
        for k in range(count):
            inverse_ref[i * count + k] = column(value, count + k)


def solve(total, base, npixels, inverse_ref):
    epochs, lanes = base.shape
    lane = iota((epochs, lanes), 1)
    covariance = jnp.concatenate([total] * (lanes // total.shape[1]), axis=1) * (1.0 / npixels)
    ends = (lane < epochs) | (lane >= lanes - epochs)
    system = base + jnp.where(ends, covariance, 0.0)
    strips = [system[i : i + 8, :] for i in range(0, epochs, 8)]
    size = 2 if epochs % 16 == 0 else 1
    for start in range(0, epochs // 8, size):
        home = range(start, start + size)
        order = [i for i in range(epochs // 8) if i not in home]
        at = lanes - epochs + start * 8
        factors = [[column(strips[i], at + k) for k in range(8 * size)] for i in order]
        values = [strips[i] for i in home]
        if inverse_ref is not None and start == 0:
            count = 8 * size
            pivots = [spread(values[k // 8], k % 8) for k in range(count)]
            values = [
                total_of([inverse_ref[i * count + k] * pivots[k] for k in range(count)])
                for i in range(size)
            ]
        else:
            values = eliminate(values, at)
        pivots = [spread(values[k // 8], k % 8) for k in range(8 * size)]
        for i, factor in zip(order, factors):
            strips[i] = strips[i] - total_of([p * q for p, q in zip(factor, pivots)])
        for i, value in zip(home, values):
            strips[i] = value
    return jnp.concatenate(strips, axis=0)


def exchange_kernel(
    n,
    hub,
    images_hbm,
    reference_hbm,
    kernels_hbm,
    index_hbm,
    mask_hbm,
    systematics_hbm,
    onsets_hbm,
    pixels,
    total_ref,
    system_ref,
    images_ref,
    reference_ref,
    kernels_ref,
    index_ref,
    mask_ref,
    systematics_ref,
    onsets_ref,
    table,
    work,
    send,
    recv,
    spare,
    packed_ref,
    early_ref,
    inverse_ref,
    load_sem,
    ready_sem,
    row_sem,
    hub_sem,
    total_sem,
    early_sem,
):
    local, rows, width = images_ref.shape
    side = kernels_hbm.shape[0]
    nk = kernels_hbm.shape[1]
    choices = kernels_ref.reshape(kernels_ref.shape[0] * nk, side)
    half = (side - 1) // 2
    tiles = width // LANES
    block = rows // n
    epochs = local * n
    nsys = systematics_ref.shape[1]
    ntr = onsets_ref.shape[0]
    columns = nsys + ntr
    pack = max(LANES // epochs, 1)
    me = lax.axis_index("ep")
    hub_send_sem, row_send_sem, total_send_sem, mate_send_sem, early_send_sem = (
        load_sem.at[i] for i in range(5)
    )
    mate = hub - 1
    pieces = recv.shape[0]
    strips = block * tiles
    share = epochs // pack
    strip = iota((share, total_ref.shape[1]), 1) // epochs

    loads = [
        pltpu.make_async_copy(source, target, load_sem.at[i])
        for i, (source, target) in enumerate(
            (
                (index_hbm, index_ref),
                (kernels_hbm, kernels_ref.at[0:side]),
                (images_hbm, images_ref),
                (mask_hbm, mask_ref),
                (reference_hbm, reference_ref),
                (systematics_hbm, systematics_ref),
                (onsets_hbm, onsets_ref),
            )
        )
    ]
    for load in loads:
        load.start()

    def signal(semaphore, device):
        pl.semaphore_signal(
            semaphore, inc=1, device_id={"ep": device}, device_id_type=pl.DeviceIdType.MESH
        )

    barrier = pltpu.get_barrier_semaphore()

    @pl.when(me == hub)
    def _():
        for d in range(1, n):
            signal(barrier, lax.rem(me + d, n))

    @pl.when(me != hub)
    def _():
        signal(barrier, hub)

    table[...] = jnp.zeros_like(table)
    for load in loads:
        load.wait()

    steps = -(-side // GROUP)
    middle, offset = half // GROUP, half % GROUP
    depth = rows * GROUP
    lane = iota((8, LANES), 1)
    sublane = iota((8, LANES), 0)
    place = lane + sublane - offset
    banks = -(-side // 8)
    pages = -(-(GROUP * side + side) // LANES)
    turned = []
    for e in range(local):
        at = e * 8 * banks
        for g in range(banks):
            table[at + 8 * g : at + 8 * g + 8, 0:side] = choices[
                pl.ds(index_ref[e] + 8 * g * nk, 8, stride=nk), :
            ]
    for e in range(local):
        at = e * 8 * banks
        turned.append(
            [
                turn(table[at + 8 * g : at + 8 * g + 8, :], 8 * g * GROUP, GROUP)
                for g in range(banks)
            ]
        )
    windows = {}
    for m in range(steps):
        for page in range(pages):
            for g in range(banks):
                low = GROUP * (8 * g + m) - page * LANES
                if low + 8 * GROUP > 0 and low < LANES:
                    away = lane - GROUP * sublane - low
                    inside = (away >= 0) & (away < GROUP) & (sublane < side - 8 * g)
                    windows[m, page, g] = inside
    flats = {}
    for m in range(steps):
        for e in range(local):
            for page in range(pages):
                total = jnp.zeros((8, LANES), jnp.float32)
                for g in range(banks):
                    if (m, page, g) in windows:
                        total = total + jnp.where(windows[m, page, g], turned[e][g], 0.0)
                total = jnp.sum(total, axis=0, keepdims=True)
                flats[e, m, page] = jnp.broadcast_to(total, (8, LANES))
    bands = [[] for _ in range(local)]
    for m in range(steps):
        for h in range(rows // 8):
            for e in range(local):
                pieces_of = []
                for start in range(0, depth, LANES):
                    base = start + GROUP * (half + m - 8 * h)
                    spot = lane + base - GROUP * sublane
                    value = jnp.zeros((8, LANES), jnp.float32)
                    for page in range(pages):
                        if base + LANES <= page * LANES or base - 7 * GROUP >= (page + 1) * LANES:
                            continue
                        moved = turn(flats[e, m, page], -base, GROUP)
                        inside = (spot >= page * LANES) & (spot < (page + 1) * LANES)
                        value = jnp.where(inside, moved, value)
                    pieces_of.append(value)
                bands[e].append(jnp.concatenate(pieces_of, axis=1))
    good = {}
    for e in range(local):
        at = table.shape[0] - (e + 1) * 8
        table[at : at + tiles, 0:rows] = mask_ref[e].astype(jnp.float32)
        for t in range(tiles):
            row = jnp.broadcast_to(table[at + t : at + t + 1, :], (8, LANES))
            for r in range(0, rows, 8):
                good[e, t, r] = jnp.take_along_axis(row, sublane + r, axis=1)
    for e in range(local):
        spread_rows = []
        for r in range(rows):
            moved = [
                turn(
                    jnp.broadcast_to(
                        images_ref[e, r : r + 1, t * LANES : (t + 1) * LANES], (8, LANES)
                    ),
                    offset,
                    -1,
                )
                for t in range(tiles)
            ]
            moved.append(None)
            parts_of = []
            for t in range(tiles + 1):
                value = jnp.zeros((8, LANES), jnp.float32) if moved[t] is None else moved[t]
                before, after = moved[t - 1], moved[(t + 1) % (tiles + 1)]
                value = jnp.where(place < 0, 0.0 if before is None else before, value)
                value = jnp.where(place >= LANES, 0.0 if after is None else after, value)
                parts_of.append(value)
            spread_rows.append(jnp.concatenate(parts_of, axis=1))
        response = dot(
            jnp.concatenate(bands[e], axis=0),
            jnp.concatenate(spread_rows, axis=0),
            ((1,), (0,)),
            lax.Precision.HIGH,
        )
        span = width + LANES
        model = response[middle * rows : (middle + 1) * rows, 0:width]
        for m in range(steps):
            if m != middle:
                part = response[m * rows : (m + 1) * rows, :]
                model = model + pltpu.roll(part, (-GROUP * (m - middle)) % span, axis=1)[:, 0:width]
        difference = reference_ref[...] - model
        for t in range(tiles):
            for r in range(0, rows, 8):
                first = (r * tiles + t) * local + e
                piece = difference[r : r + 8, t * LANES : (t + 1) * LANES]
                send[pl.ds(first, 8, stride=tiles * local), :] = piece * good[e, t, r]

    sources = send.reshape(rows * tiles, local, LANES)
    def copy(source, target, semaphores, device):
        return pltpu.make_async_remote_copy(
            src_ref=source,
            dst_ref=target,
            send_sem=semaphores[0],
            recv_sem=semaphores[1],
            device_id={"ep": device},
            device_id_type=pl.DeviceIdType.MESH,
        )

    @pl.when(me != hub)
    def _():
        pl.semaphore_wait(barrier, 1)
        copy(sources, recv.at[:, me], (hub_send_sem, hub_sem.at[me // (n // 2)]), hub).start()

    @pl.when(me == hub)
    def _():
        pl.semaphore_wait(barrier, n - 1)
        for d in range(1, n):
            signal(ready_sem, lax.rem(me + d, n))
        recv[:, me] = sources[...]

    work[...] = jnp.zeros_like(work)
    epoch = iota((epochs, LANES), 0).astype(jnp.float32)
    template = iota((epochs, LANES), 1)
    onset = jnp.zeros((epochs, LANES), jnp.float32)
    for k in range(ntr):
        onset = jnp.where(template == k, onsets_ref[k].astype(jnp.float32), onset)
    delays = epoch - onset
    timescale = (template.astype(jnp.float32) + 1.0) * epochs / (2.0 * ntr)
    transient = jnp.where(delays >= 0.0, jnp.exp(-jnp.maximum(delays, 0.0) / timescale), 0.0)
    work[:, epochs : epochs + nsys] = systematics_ref[...]
    work[:, epochs + nsys : epochs + columns] = transient[:, 0:ntr]
    design = work[...]
    outer = dot(design, design, ((1,), (1,)))
    diagonal = iota((epochs, epochs), 0) == iota((epochs, epochs), 1)
    ridge = jnp.where(diagonal, cov_ridge, 0.0)
    lanes = work.shape[1]
    work[:, 0:epochs] = ridge
    work[:, lanes - epochs : lanes] = fit_ridge * outer + ridge

    def drain(ref, semaphore):
        pltpu.make_async_copy(ref, ref, semaphore).wait()

    @pl.when(me != hub)
    def _():
        pl.semaphore_wait(ready_sem, 1)

    for d in range(n - 2):
        device = 2 + lax.rem(me + d, n - 2)

        @pl.when(me != device)
        def _():
            rows_of = sources.at[pl.ds(device * strips, strips)]
            copy(rows_of, pixels.at[:, me], (row_send_sem, row_sem), device).start()

    @pl.when(me > hub)
    def _():
        pixels[:, me] = sources[pl.ds(me * strips, strips)]

    count = early_ref.shape[0]
    early = count * 2 == epochs
    gathered = recv.reshape(pieces, epochs, LANES)

    @pl.when(me == hub)
    def _():
        drain(recv.at[:, 0 : n // 2 - 1], hub_sem.at[0])
        if early:
            data = jnp.concatenate([gathered[i, 0:count, :] for i in range(pieces)], axis=1)
            both = jnp.concatenate(cut(data, 2), axis=0)
            square = plain_dot(both, both, ((1,), (1,)))
            early_ref[...] = jnp.zeros_like(early_ref)
            early_ref[:, 0 : 2 * count] = square[0:count] + square[count : 2 * count]
            for d in range(1, n):
                device = lax.rem(me + n - d, n)
                copy(early_ref, early_ref, (early_send_sem, early_sem), device).start()

    if early:

        @pl.when(me != hub)
        def _():
            drain(early_ref, early_sem)

        invert_early(early_ref[...], work[...], float(rows * width), inverse_ref)

    @pl.when(me == hub)
    def _():
        drain(recv.at[:, 0 : n // 2], hub_sem.at[1])
        copy(recv.at[mate * strips : hub * strips], pixels, (row_send_sem, row_sem), mate).start()
        step = min(pieces, 32)

        def gram(start):
            data = jnp.concatenate([gathered[start + i] for i in range(step)], axis=1)
            both = jnp.concatenate(cut(data, 2), axis=0)
            square = plain_dot(both, both, ((1,), (1,)))
            return square[0:epochs] + square[epochs : 2 * epochs]

        if step == pieces:
            square = gram(0)
        else:
            square = lax.fori_loop(
                0,
                pieces // step,
                lambda i, value: value + gram(i * step),
                jnp.zeros((epochs, 2 * epochs), jnp.float32),
            )
        if pack > 1:
            table[0:epochs, 2 * epochs :] = jnp.zeros((epochs, LANES - 2 * epochs), jnp.float32)
            table[0:epochs, 0 : 2 * epochs] = square
            wide = table[0:epochs, :]
            total = wide
            for j in range(1, pack):
                total = total + pltpu.roll(wide, j * epochs, axis=1)
            total_ref[...] = total
            packed = total[0:share, :]
            for j in range(1, pack):
                packed = jnp.where(strip == j, total[j * share : (j + 1) * share, :], packed)
            packed_ref[...] = packed
        else:
            total_ref[...] = square[:, 0:epochs] + square[:, epochs : 2 * epochs]
        for d in range(1, n):
            device = lax.rem(me + n - d, n)
            if d == 1 and pack > 1:
                copy(total_ref, total_ref, (mate_send_sem, total_sem), device).start()
            elif pack > 1:
                copy(packed_ref, packed_ref, (total_send_sem, total_sem), device).start()
            else:
                copy(total_ref, total_ref, (total_send_sem, total_sem), device).start()
        pixels[...] = recv[hub * strips : (hub + 1) * strips]

    @pl.when(me == mate)
    def _():
        drain(total_ref, total_sem)

    @pl.when(me > hub)
    def _():
        if pack > 1:
            drain(packed_ref, total_sem)
            packed = packed_ref[...]
            for j in range(pack):
                one = jnp.where(strip == j, packed, 0.0)
                total = one
                for k in range(1, pack):
                    total = total + pltpu.roll(one, k * epochs, axis=1)
                total_ref[j * share : (j + 1) * share, :] = total
        else:
            drain(total_ref, total_sem)

    system_ref[...] = solve(
        total_ref[...], work[...], float(rows * width), inverse_ref if early else None
    )

    @pl.when(me == mate)
    def _():
        drain(sources, hub_send_sem)
        drain(pixels, row_sem)
        drain(pixels.at[:, 0 : n - 2], row_send_sem)

    @pl.when(me > hub)
    def _():
        drain(sources, hub_send_sem)
        drain(pixels.at[:, 0 : n - 1], row_sem)
        drain(pixels.at[:, 0 : n - 3], row_send_sem)

    @pl.when(me == hub)
    def _():
        drain(recv.at[0 : 2 * strips, 0 : n - 1], row_send_sem)
        if early:
            drain(recv.at[0 : count // local, 0 : n - 1], early_send_sem)
        if pack > 1:
            drain(spare.at[0 : n - 2], total_send_sem)
            drain(total_ref, mate_send_sem)
        else:
            drain(spare.at[0 : n - 1], total_send_sem)


def split_dot(a, b):
    high, low = cut(a, 2)
    left = jnp.concatenate([high, high, low, low], axis=0)
    high, low = cut(b, 2)
    right = jnp.concatenate([high, low, high, low], axis=0)
    return plain_dot(left, right, ((0,), (0,)))


def fit_kernel(npixels, pixels_ref, total_ref, system_ref, coefficients_ref, epoch_ref):
    columns, block, width = coefficients_ref.shape
    strips, n, local, _ = pixels_ref.shape
    epochs = n * local
    rows_of = pixels_ref.reshape(strips, epochs, LANES)
    data = jnp.concatenate([rows_of[i] for i in range(strips)], axis=1)
    total = total_ref[...]
    system = system_ref[...]

    solved = system[:, 0:LANES] if epochs < LANES else system[:, 0:epochs]
    scatter = total[:, 0:epochs]
    if epochs * 4 == total.shape[1]:
        high, low = (part.astype(jnp.float32) for part in cut(total, 2))
        block_of = iota(total.shape, 1) // epochs
        left = jnp.where(block_of < 2, high, low).astype(jnp.bfloat16)
        high, low = cut(solved, 2)
        right = jnp.concatenate([high, low, high, low], axis=0)
        product = plain_dot(left, right, ((1,), (0,))) * solved
    else:
        product = dot(scatter, solved, ((1,), (0,))) * solved
    epoch_ref[...] = (jnp.sum(product, axis=0, keepdims=True) * (1.0 / npixels))[0, 0:epochs]

    if 4 * epochs <= 256:
        fitted = split_dot(system, data)
    else:
        fitted = dot(system, data, ((0,), (0,)))
    fitted = fitted[epochs : epochs + columns, :]
    for q in range(block):
        coefficients_ref[:, q, :] = fitted[:, q * width : (q + 1) * width]


HUB = 1
EARLY = 16


def ceil_to(value, unit):
    return -(-value // unit) * unit


def solution(mesh):
    n = mesh.shape["ep"]

    def shards(images, reference_image, kernels, kernel_index, tile_mask, systematics, onsets):
        local, rows, width = images.shape
        side = kernels.shape[1]
        tiles = width // LANES
        block = rows // n
        epochs = local * n
        columns = systematics.shape[1] + onsets.shape[0]
        pack = max(LANES // epochs, 1)
        share = epochs // pack
        part_lanes = max(LANES, epochs)
        vmem = pl.BlockSpec(memory_space=pltpu.VMEM)
        dma = pltpu.SemaphoreType.DMA
        f32 = jnp.float32
        flat_kernels = jnp.transpose(kernels, (1, 0, 2))
        flat_mask = jnp.transpose(tile_mask, (0, 2, 1))
        system_lanes = ceil_to(2 * epochs + columns, LANES)
        pieces = rows * tiles
        strips = block * tiles
        pixels, total, system = pl.pallas_call(
            functools.partial(exchange_kernel, n, HUB),
            out_shape=(
                jax.ShapeDtypeStruct((strips, n, local, LANES), f32),
                jax.ShapeDtypeStruct((epochs, part_lanes), f32),
                jax.ShapeDtypeStruct((epochs, system_lanes), f32),
            ),
            in_specs=[pl.BlockSpec(memory_space=pltpu.HBM)] * 7,
            out_specs=(vmem, vmem, vmem),
            scratch_shapes=[
                pltpu.VMEM(images.shape, f32),
                pltpu.VMEM(reference_image.shape, f32),
                pltpu.VMEM((ceil_to(side, 8), *flat_kernels.shape[1:]), f32),
                pltpu.SMEM(kernel_index.shape, jnp.int32),
                pltpu.VMEM(flat_mask.shape, jnp.int32),
                pltpu.VMEM(systematics.shape, f32),
                pltpu.SMEM(onsets.shape, jnp.int32),
                pltpu.VMEM((max(LANES, local * ceil_to(side + 8, 8)), LANES), f32),
                pltpu.VMEM((epochs, system_lanes), f32),
                pltpu.VMEM((rows * tiles * local, LANES), f32),
                pltpu.VMEM((pieces, n, local, LANES), f32),
                pltpu.VMEM((n, share, part_lanes), f32),
                pltpu.VMEM((share, part_lanes), f32),
                pltpu.VMEM((EARLY, LANES), f32),
                pltpu.VMEM((2 * EARLY, 8, LANES), f32),
                pltpu.SemaphoreType.DMA((7,)),
                pltpu.SemaphoreType.REGULAR,
                dma,
                pltpu.SemaphoreType.DMA((2,)),
                dma,
                dma,
            ],
            compiler_params=pltpu.CompilerParams(
                collective_id=0, has_side_effects=True, vmem_limit_bytes=VMEM_GRANT
            ),
        )(
            *(
                pltpu.with_memory_space_constraint(value, pltpu.HBM)
                for value in (
                    images,
                    reference_image,
                    flat_kernels,
                    kernel_index,
                    flat_mask,
                    systematics,
                    onsets,
                )
            )
        )
        return pl.pallas_call(
            functools.partial(fit_kernel, float(rows * width)),
            out_shape=(
                jax.ShapeDtypeStruct((columns, block, width), f32),
                jax.ShapeDtypeStruct((epochs,), f32),
            ),
            in_specs=[vmem, vmem, vmem],
            out_specs=(vmem, vmem),
            compiler_params=pltpu.CompilerParams(vmem_limit_bytes=VMEM_GRANT),
        )(pixels, total, system)

    in_specs = (
        P(("field", "ep"), None, None),
        P("field", None),
        P(),
        P(("field", "ep")),
        P(("field", "ep"), None, None),
        P("field", None),
        P("field"),
    )
    out_specs = (P(None, ("field", "ep"), None), P("field"))
    return jax.shard_map(shards, mesh=mesh, in_specs=in_specs, out_specs=out_specs, check_vma=False)
```
